32 devices in a mesh: row: 4 (over z), col: 4 (over y, x), layer: 2 (over core).
Axes of the slice: x: 2, y: 2, z: 4, core: 2. Of those that a mesh axis runs over, the one named last changes fastest.
Arguments:
- matrix: float32 [16, 512, 16, 512], P('row', None, 'col', 'layer'), may hold values from -40 to 40, as said below
- transforms: float32 [1, 8, 1024, 1024], P(None, 'row', ('col', 'layer')), may hold values from -0.1875 to 0.1875
Outputs:
- swept: float32 [16, 512, 16, 512], P('row', None, 'col', 'layer')
The draws below stay inside these ranges and needn't reach their ends.
Inputs may be any that keep to these rules, and one draw needn't show every extreme that they name: `matrix`: symmetric: entry [i, a, j, b] equals entry [j, b, i, a].
All inputs are finite; a program needn't handle non-finite values.
Results may differ from the reference program's by a relative error of at most 0.0001.
Values sent between devices are 32-bit elements; how exact they have to be, the bound alone decides.
A program may use at most 192 MiB of HBM per device.

```python
import jax
import jax.numpy as jnp
from jax import lax

BS = 512
STEPS = 1
PAIRS = 8
NBLK = 16


def draw_matrix(key, part):
    gaussian = jax.random.normal(key, (NBLK * BS, NBLK * BS), jnp.float32)
    symmetric = (gaussian + gaussian.T) * 0.7071067811865476
    return symmetric.reshape(NBLK, BS, NBLK, BS)


def steps_of(own_key, dims, pieces, low, largest):
    def one(position, parts):
        heights = jax.random.uniform(jax.random.fold_in(jax.random.fold_in(own_key, 6), position), (parts,), jnp.float32, low / len(pieces), largest / len(pieces))
        return jnp.repeat(jnp.exp(heights), dims[position] // parts).reshape((-1,) + (1,) * (len(dims) - position - 1))

    factor_of = one(*pieces[0])
    for cut in pieces[1:]:
        factor_of = factor_of * one(*cut)
    return factor_of


def centred(own_key, dims, spread, limit, pieces=(), held_as=jnp.bfloat16):
    loudness = steps_of(own_key, dims, pieces, -0.22, 0.18) if pieces else 1.0
    result = jax.random.normal(own_key, dims, jnp.float32) * spread * loudness
    return jnp.minimum(jnp.maximum(result, -limit), limit).astype(held_as)


def setup_inputs(seed: int = 0) -> dict:
    keys = jax.random.split(jax.random.key(seed), 3)
    matrix = draw_matrix(jax.random.fold_in(keys[2], 71), 0)
    transforms = centred(keys[1], (STEPS, PAIRS, 2 * BS, 2 * BS), (2 * BS) ** -0.5, 0.1875, ((1, 4), (2, 8)), jnp.float32)
    return dict(matrix=matrix, transforms=transforms)


def sweep_order(count):
    slot_ids = jnp.arange(count, dtype=jnp.int32)
    is_odd = slot_ids % 2
    source = jnp.where(is_odd == 0, slot_ids - 2, slot_ids + 2)
    source = jnp.where(slot_ids == 0, 0, source)
    source = jnp.where(slot_ids == 2, 1, source)
    source = jnp.where(slot_ids == count - 1, count - 2, source)
    return source.astype(jnp.int32)


def reference(matrix, transforms):
    source = sweep_order(NBLK)
    current = matrix
    for step_index in range(STEPS):
        blocks = transforms[step_index]
        grouped = current.reshape(PAIRS, 2 * BS, PAIRS, 2 * BS)
        left_part = jnp.einsum("pkqb,pka->paqb", grouped, blocks, precision=lax.Precision.HIGHEST)
        rotated_pairs = jnp.einsum("paqk,qkb->paqb", left_part, blocks, precision=lax.Precision.HIGHEST)
        rotated = rotated_pairs.reshape(NBLK, BS, NBLK, BS)
        current = jnp.take(jnp.take(rotated, source, axis=0), source, axis=2)
    return current
```

```python
import functools

import jax
import jax.numpy as jnp
from jax import lax
from jax.experimental import pallas as pl
from jax.experimental.pallas import tpu as pltpu
from jax.sharding import PartitionSpec as P

MESH = pl.DeviceIdType.MESH
LANES = 128
ROWS = 128
VMEM_LIMIT = 66_000_000


def halves_of(x):
    high = x.astype(jnp.bfloat16)
    low = (x - high.astype(jnp.float32)).astype(jnp.bfloat16)
    return high, low


def three_dots(a_high, a_low, b_high, b_low):
    def dot(a, b):
        return lax.dot_general(a, b, (((1,), (0,)), ((), ())), preferred_element_type=jnp.float32)

    return dot(a_high, b_high) + (dot(a_high, b_low) + dot(a_low, b_high))


def sweep(
    size,
    a_ref, t_ref,
    out_ref, ap_ref, jr_ref, z_ref, jc_ref, lr_ref,
    a_hi, a_lo, jt_hi, jt_lo, jc_hi, jc_lo, lr_hi, lr_lo, l_tile, o_tile,
    own_v, a_stage, j_stage, c_stage, l_stage,
    stage_sem, own_sem,
    ap_send, ap_recv, jr_send, jr_recv,
    zu_send, zu_recv, zd_send, zd_recv,
    ju_send, jd_send, jc_recv, jp_send, jp_recv,
    lr_send, lr_recv, o_send, o_recv,
):
    rows_n, cols_n, pair_dev, width, block, half, piece = size
    order = 2 * block
    tiles = half // LANES
    per_row = width * tiles
    r = lax.axis_index("row")
    c = lax.axis_index("col")
    l = lax.axis_index("layer")
    other = 1 - l
    partner = (r, c, other)
    pending = []

    def remote(src, dst, send, recv, device):
        return pltpu.make_async_remote_copy(
            src_ref=src, dst_ref=dst, send_sem=send, recv_sem=recv, device_id=device, device_id_type=MESH
        )

    def send(copy, condition=None):
        if condition is None:
            copy.start()
        else:
            pl.when(condition)(copy.start)
        pending.append((copy, condition))

    def lanes(start, count):
        return pl.ds(pl.multiple_of(start, LANES), count)

    barrier = pltpu.get_barrier_semaphore()
    for mask in range(cols_n):
        for layer in (l, other):
            if mask == 0 and layer is l:
                continue
            pl.semaphore_signal(barrier, inc=1, device_id=(r, c ^ mask, layer), device_id_type=MESH)
    has_next = r + 1 < rows_n
    has_prev = r > 0

    @pl.when(has_next)
    def _():
        pl.semaphore_signal(barrier, inc=1, device_id=(r + 1, c, l), device_id_type=MESH)

    @pl.when(has_prev)
    def _():
        pl.semaphore_signal(barrier, inc=1, device_id=(r - 1, c, l), device_id_type=MESH)

    pl.semaphore_wait(barrier, 2 * cols_n - 1 + has_next.astype(jnp.int32) + has_prev.astype(jnp.int32))

    for p in range(pair_dev):
        send(remote(t_ref.at[p], z_ref.at[r, p], zu_send.at[0, p], zu_recv.at[1, p], (r + 1, c, l)), has_next)
        send(remote(t_ref.at[p], z_ref.at[r, p], zd_send.at[0, p], zd_recv.at[1, p], (r - 1, c, l)), has_prev)

    def part(m, layer):
        return lanes(m * block + layer * half, half)

    mine = c * 2 + l
    for mask in list(range(1, cols_n)) + [0]:
        for s, layer in ((0, l), (1, other)):
            if mask == 0 and s == 0:
                continue
            for m in range(2):
                send(remote(
                    t_ref.at[:, :, part(m, layer)],
                    jr_ref.at[:, m, pl.ds(mine * piece, piece), :],
                    jr_send.at[mask, s, m], jr_recv.at[mask, s, m], (r, c ^ mask, layer),
                ))

    raw = pair_dev * order * per_row // pair_dev
    for p in range(pair_dev):
        rows = pl.ds(p * raw, raw)
        send(remote(a_ref.at[rows, :], ap_ref.at[rows, :], ap_send.at[p], ap_recv.at[p], partner))

    for p in range(pair_dev):
        send(remote(
            t_ref.at[p], jc_ref.at[mine, p], ju_send.at[0, p], jc_recv.at[c ^ r, p], (r, r, l)
        ), c != r)

    load = pltpu.make_async_copy(t_ref, own_v, own_sem.at[0])
    load.start()
    load.wait()
    fills = [pltpu.make_async_copy(own_v, z_ref.at[r], own_sem.at[0])]
    for m in range(2):
        fills.append(pltpu.make_async_copy(
            own_v.at[:, :, part(m, l)], jr_ref.at[:, m, pl.ds(mine * piece, piece), :], own_sem.at[1 + m]
        ))
    for copy in fills:
        copy.start()

    def split_columns(src, layer, first):
        chunk = ROWS * per_row
        count = order // ROWS

        def fetch(at):
            slot = lax.rem(at, 2)
            rows = pl.ds(pl.multiple_of((first + at) * chunk, chunk), chunk)
            return pltpu.make_async_copy(src.at[rows, :], a_stage.at[slot], stage_sem.at[slot])

        fetch(0).start()

        def body(at, carry):
            @pl.when(at + 1 < count)
            def _():
                fetch(at + 1).start()

            fetch(at).wait()
            slot = lax.rem(at, 2)
            rows = pl.ds(pl.multiple_of(at * ROWS, ROWS), ROWS)
            for j in range(width):
                for tile in range(tiles):
                    x = a_stage[slot, pl.ds(tile * width + j, ROWS, per_row), :]
                    high, low = halves_of(x)
                    cols = lanes(j * block + layer * half + tile * LANES, LANES)
                    a_hi[first // count, rows, cols] = high
                    a_lo[first // count, rows, cols] = low
            return carry

        lax.fori_loop(0, count, body, 0)

    for p in range(pair_dev):
        split_columns(a_ref, l, p * (order // ROWS))
    for copy in fills:
        copy.wait()
    for p in range(pair_dev):
        rows = pl.ds(p * raw, raw)
        remote(a_ref.at[rows, :], ap_ref.at[rows, :], ap_send.at[p], ap_recv.at[p], partner).wait_recv()
        split_columns(ap_ref, other, p * (order // ROWS))

    def forward(step):
        for p in range(pair_dev):
            for recv, snd, plane, to, into in (
                (zu_recv, zu_send, r - step, r + 1, ju_send),
                (zd_recv, zd_send, r + step, r - 1, jd_send),
            ):
                here = (plane >= 0) & (plane < rows_n)
                onward = here & (to >= 0) & (to < rows_n)
                at = jnp.clip(plane, 0, rows_n - 1)
                block_ref = z_ref.at[at, p]

                @pl.when(here)
                def _():
                    remote(block_ref, block_ref, snd.at[step, p], recv.at[step, p], partner).wait_recv()

                if step + 1 < rows_n:
                    send(remote(block_ref, block_ref, snd.at[step, p], recv.at[step + 1, p], (to, c, l)), onward)
                send(remote(
                    block_ref, jc_ref.at[mine, p], into.at[step, p], jc_recv.at[c ^ at, p], (r, at, l)
                ), here & (at != c))

    early = max(rows_n - 2, 1)
    forward(1)

    wide = 2 * piece
    for mask in range(cols_n):
        for s, layer in ((0, l), (1, other)):
            if mask == 0 and s == 0:
                continue
            for m in range(2):
                sender = (c ^ mask) * 2 + layer
                remote(
                    t_ref.at[:, :, part(m, layer)],
                    jr_ref.at[:, m, pl.ds(sender * piece, piece), :],
                    jr_send.at[mask, s, m], jr_recv.at[mask, s, m], partner,
                ).wait_recv()
        at = lanes((c ^ mask) * wide, wide)
        fetch = pltpu.make_async_copy(jr_ref.at[:, :, at, :], j_stage, stage_sem.at[0])
        fetch.start()
        fetch.wait()

        def turn(index, carry):
            p, m = lax.div(index, 2), lax.rem(index, 2)
            high, low = halves_of(j_stage[p, m].T)
            jt_hi[index, :, at] = high
            jt_lo[index, :, at] = low
            return carry

        lax.fori_loop(0, width, turn, 0)

    for step in range(2, early + 1):
        forward(step)

    def left(slot):
        p = slot // 2
        if slot == 1:
            moved, target, at = has_prev, r - 1, jnp.where(has_prev, 3, 2)
        elif slot == width - 2:
            moved, target, at = has_next, r + 1, jnp.where(has_next, 0, 3)
        else:
            moved, target, at = None, r, (jnp.where(has_prev, 2, 0) if slot == 0 else 1)

        def copies(n):
            src, dst = l_tile.at[slot * width + n], lr_ref.at[at, n]
            there = remote(src, dst, lr_send.at[slot, n], lr_recv.at[at, n], (target, c, l))
            here = pltpu.make_async_copy(src, dst, lr_recv.at[at, n])
            return there, here

        def body(n, carry):
            cols = lanes(n * block, block)
            l_tile[slot * width + n] = three_dots(
                jt_hi[slot], jt_lo[slot], a_hi[p, :, cols], a_lo[p, :, cols]
            )
            there, here = copies(n)
            if moved is None:
                here.start()
            else:
                pl.when(moved)(there.start)
                pl.when(jnp.logical_not(moved))(here.start)
            return carry

        lax.fori_loop(0, width, body, 0)
        if moved is not None:
            for n in range(width):
                pending.append((copies(n)[0], moved))

    left(width - 2)
    left(1)
    left(0)
    left(width - 1)
    for step in range(early + 1, rows_n):
        forward(step)

    def right_pieces(p):
        todo = []
        for mask in list(range(1, cols_n)) + [0]:
            index = (c ^ mask) * 2 + l
            src = jc_ref.at[index, p] if mask else z_ref.at[c, p]
            if mask:
                remote(src, src, jp_send.at[mask, p], jc_recv.at[mask, p], partner).wait_recv()
            copy = remote(src, jc_ref.at[index, p], jp_send.at[mask, p], jp_recv.at[mask, p], partner)
            send(copy)
            todo.append((src, index, None))
        for mask in list(range(1, cols_n)) + [0]:
            index = (c ^ mask) * 2 + other
            src = jc_ref.at[index, p]
            todo.append((src, index, remote(src, src, jp_send.at[mask, p], jp_recv.at[mask, p], partner)))

        def fetch(n):
            src, _, copy = todo[n]
            if copy is not None:
                copy.wait_recv()
            load = pltpu.make_async_copy(src, c_stage.at[n % 2], stage_sem.at[n % 2])
            load.start()
            return load

        loads = [fetch(0)]
        for n, (_, index, _) in enumerate(todo):
            if n + 1 < len(todo):
                loads.append(fetch(n + 1))
            loads[n].wait()
            high, low = halves_of(c_stage[n % 2])
            rows = pl.ds(pl.multiple_of(index * piece, piece), piece)
            jc_hi[p, rows, :] = high
            jc_lo[p, rows, :] = low

    def left_rows(at):
        def fetch(n):
            slot = lax.rem(n, 2)
            return pltpu.make_async_copy(lr_ref.at[at, n], l_stage.at[slot], stage_sem.at[slot])

        def arrived(n):
            pltpu.make_async_copy(lr_ref.at[at, n], lr_ref.at[at, n], lr_recv.at[at, n]).wait()

        arrived(0)
        fetch(0).start()

        def body(n, carry):
            @pl.when(n + 1 < width)
            def _():
                arrived(n + 1)
                fetch(n + 1).start()

            fetch(n).wait()
            high, low = halves_of(l_stage[lax.rem(n, 2)])
            cols = lanes(n * block, block)
            lr_hi[at, :, cols] = high
            lr_lo[at, :, cols] = low
            return carry

        lax.fori_loop(0, width, body, 0)

    left_end, right_end = c > 0, c + 1 < cols_n

    def right(at, j):
        q, m = j // 2, j % 2
        rows = slice(q * order, (q + 1) * order)
        cols = slice(m * block, (m + 1) * block)
        tile = at * width + j
        o_tile[tile] = three_dots(
            lr_hi[at, :, rows], lr_lo[at, :, rows], jc_hi[q, :, cols], jc_lo[q, :, cols]
        )
        if j == 1:
            moved, target, slot = left_end, c - 1, jnp.where(left_end, 3, 2)
        elif j == width - 2:
            moved, target, slot = right_end, c + 1, jnp.where(right_end, 0, 3)
        else:
            moved, target, slot = None, c, (jnp.where(left_end, 2, 0) if j == 0 else 1)
        dst = out_ref.at[slot, at, pl.ds(pl.multiple_of(l * half, half), half), :]
        column = c if moved is None else jnp.where(moved, target, c)
        for s, layer in ((0, l), (1, other)):
            src = o_tile.at[tile, :, lanes(layer * half, half)]
            there = remote(src, dst, o_send.at[tile, s], o_recv.at[slot, l], (r, column, layer))
            if s == 1:
                send(there)
                continue
            here = pltpu.make_async_copy(src, dst, o_recv.at[slot, l])
            if moved is None:
                here.start()
            else:
                send(there, moved)
                pl.when(jnp.logical_not(moved))(here.start)

    staying, arriving = (1, width - 2), (0, width - 1)
    for at in staying:
        left_rows(at)
    for q in range(pair_dev):
        right_pieces(q)
        for at in staying:
            for j in ((1, 0) if q == 0 else (2, 3)):
                right(at, j)
    for at in arriving:
        left_rows(at)
        for j in (1, 2, 0, 3):
            right(at, j)

    for slot in range(width):
        for layer in range(2):
            block_ref = out_ref.at[slot, :, pl.ds(layer * half, half), :]
            pltpu.make_async_copy(block_ref, block_ref, o_recv.at[slot, layer]).wait()
    for copy, condition in pending:
        if condition is None:
            copy.wait_send()
        else:
            pl.when(condition)(copy.wait_send)


def spread(width, tiles, x_ref, o_ref):
    rows = x_ref.shape[2]
    for j in range(width):
        for tile in range(tiles):
            o_ref[pl.ds(tile * width + j, rows, width * tiles), :] = x_ref[j, 0, :, tile * LANES : (tile + 1) * LANES]


def shards(matrix, transforms):
    width, block, _, half = matrix.shape
    pair_dev = width // 2
    order = 2 * block
    rows_n, cols_n = lax.axis_size("row"), lax.axis_size("col")
    tiles = half // LANES
    per_row = width * tiles
    raw_rows = width * block * per_row
    own = transforms[0]
    piece = own.shape[1]
    pieces = 2 * cols_n
    f32, bf16 = jnp.float32, jnp.bfloat16

    raw = matrix.reshape(width * block, width, tiles, LANES).transpose(0, 2, 1, 3).reshape(raw_rows, LANES)
    any_space = pl.BlockSpec(memory_space=pl.ANY)
    dma = pltpu.SemaphoreType.DMA
    flops = 3 * 2 * 2 * width * half * order * width * block
    outs = pl.pallas_call(
        functools.partial(sweep, (rows_n, cols_n, pair_dev, width, block, half, piece)),
        name="sweep",
        out_shape=[
            jax.ShapeDtypeStruct((width, width, block, half), f32),
            jax.ShapeDtypeStruct((raw_rows, LANES), f32),
            jax.ShapeDtypeStruct((pair_dev, 2, order, half), f32),
            jax.ShapeDtypeStruct((rows_n, pair_dev, piece, order), f32),
            jax.ShapeDtypeStruct((pieces, pair_dev, piece, order), f32),
            jax.ShapeDtypeStruct((width, width, half, block), f32),
        ],
        in_specs=[any_space, any_space],
        out_specs=[any_space] * 6,
        scratch_shapes=[
            pltpu.VMEM((pair_dev, order, width * block), bf16),
            pltpu.VMEM((pair_dev, order, width * block), bf16),
            pltpu.VMEM((width, half, order), bf16),
            pltpu.VMEM((width, half, order), bf16),
            pltpu.VMEM((pair_dev, order, order), bf16),
            pltpu.VMEM((pair_dev, order, order), bf16),
            pltpu.VMEM((width, half, width * block), bf16),
            pltpu.VMEM((width, half, width * block), bf16),
            pltpu.VMEM((width * width, half, block), f32),
            pltpu.VMEM((width * width, half, block), f32),
            pltpu.VMEM((pair_dev, piece, order), f32),
            pltpu.VMEM((2, ROWS * per_row, LANES), f32),
            pltpu.VMEM((pair_dev, 2, 2 * piece, half), f32),
            pltpu.VMEM((2, piece, order), f32),
            pltpu.VMEM((2, half, block), f32),
            dma((2,)), dma((3,)),
            dma((pair_dev,)), dma((pair_dev,)),
            dma((cols_n, 2, 2)), dma((cols_n, 2, 2)),
            dma((rows_n, pair_dev)), dma((rows_n, pair_dev)), dma((rows_n, pair_dev)), dma((rows_n, pair_dev)),
            dma((rows_n, pair_dev)), dma((rows_n, pair_dev)), dma((cols_n, pair_dev)),
            dma((cols_n, pair_dev)), dma((cols_n, pair_dev)),
            dma((width, width)), dma((width, width)),
            dma((width * width, 2)), dma((width, 2)),
        ],
        compiler_params=pltpu.CompilerParams(
            collective_id=0, has_side_effects=True, vmem_limit_bytes=VMEM_LIMIT
        ),
        cost_estimate=pl.CostEstimate(flops=flops, bytes_accessed=0, transcendentals=0),
    )(raw, own)
    blocks = outs[0]

    rows = 256
    steps = block // rows
    result = pl.pallas_call(
        functools.partial(spread, width, tiles),
        name="spread",
        grid=(width, steps),
        in_specs=[pl.BlockSpec((width, 1, rows, half), lambda i, a: (0, i, a, 0))],
        out_specs=pl.BlockSpec((rows * per_row, LANES), lambda i, a: (i * steps + a, 0)),
        out_shape=jax.ShapeDtypeStruct((raw_rows, LANES), f32),
    )(blocks)
    result = result.reshape(width, block, tiles, width, LANES).transpose(0, 1, 3, 2, 4)
    return result.reshape(width, block, width, half)


def solution(mesh):
    return jax.shard_map(
        shards,
        mesh=mesh,
        in_specs=(P("row", None, "col", "layer"), P(None, "row", ("col", "layer"), None)),
        out_specs=P("row", None, "col", "layer"),
        check_vma=False,
    )
```

```python
import functools

import jax
import jax.numpy as jnp
from jax import lax
from jax.experimental import pallas as pl
from jax.experimental.pallas import tpu as pltpu
from jax.sharding import PartitionSpec as P

MESH = pl.DeviceIdType.MESH
LANES = 128
ROWS = 256
VMEM_LIMIT = 66_000_000
scope = jax.named_scope


def halves_of(x):
    high = x.astype(jnp.bfloat16)
    low = (x - high.astype(jnp.float32)).astype(jnp.bfloat16)
    return high, low


def three_dots(a_high, a_low, b_high, b_low):
    def dot(a, b):
        return lax.dot_general(a, b, (((1,), (0,)), ((), ())), preferred_element_type=jnp.float32)

    return dot(a_high, b_high) + (dot(a_high, b_low) + dot(a_low, b_high))


def sweep(
    size,
    a_ref, t_ref,
    out_ref, ap_ref, jr_ref, jo_ref, z_ref, jc_ref, lr_ref, via_ref,
    a_hi, a_lo, jt_hi, jt_lo, jc_hi, jc_lo, lr_hi, lr_lo, l_tile, o_tile,
    own_v, a_stage, j_stage, c_stage, l_stage,
    stage_sem, c_sem, own_sem,
    ap_send, ap_recv, jr_send, jr_recv,
    zu_send, zu_recv, zd_send, zd_recv,
    ju_send, jd_send, jc_recv, jp_send, jp_recv, jo_send, jo_recv,
    lr_send, lr_recv, o_send, o_recv, via_send, via_recv,
):
    rows_n, cols_n, pair_dev, width, block, half, piece = size
    order = 2 * block
    tiles = half // LANES
    r = lax.axis_index("row")
    c = lax.axis_index("col")
    l = lax.axis_index("layer")
    other = 1 - l
    partner = (r, c, other)
    mine = c * 2 + l
    square = cols_n == 4
    pending = []

    def remote(src, dst, send, recv, device):
        return pltpu.make_async_remote_copy(
            src_ref=src, dst_ref=dst, send_sem=send, recv_sem=recv, device_id=device, device_id_type=MESH
        )

    def send(copy, condition=None):
        if condition is None:
            copy.start()
        else:
            pl.when(condition)(copy.start)
        pending.append((copy, condition))

    def lanes(start, count):
        return pl.ds(pl.multiple_of(start, LANES), count)

    def member(s, p):
        return 1 - p if s == 0 else p

    def slot_of(s, p):
        return 2 * p + member(s, p)

    barrier = pltpu.get_barrier_semaphore()
    for mask in range(cols_n):
        for layer in (l, other):
            if mask == 0 and layer is l:
                continue
            pl.semaphore_signal(barrier, inc=1, device_id=(r, c ^ mask, layer), device_id_type=MESH)
    has_next = r + 1 < rows_n
    has_prev = r > 0

    @pl.when(has_next)
    def _():
        pl.semaphore_signal(barrier, inc=1, device_id=(r + 1, c, l), device_id_type=MESH)

    @pl.when(has_prev)
    def _():
        pl.semaphore_signal(barrier, inc=1, device_id=(r - 1, c, l), device_id_type=MESH)

    with scope("barrier"):
        pl.semaphore_wait(barrier, 2 * cols_n - 1 + has_next.astype(jnp.int32) + has_prev.astype(jnp.int32))

    def own_half(s, p):
        return t_ref.at[p, :, pl.ds(member(s, p) * block, block)]

    def rows_out(s):
        for p in range(pair_dev):
            send(remote(
                own_half(s, p), z_ref.at[r, s, p], zu_send.at[0, s, p], zu_recv.at[1, s, p], (r + 1, c, l)
            ), has_next)
            send(remote(
                own_half(s, p), z_ref.at[r, s, p], zd_send.at[0, s, p], zd_recv.at[1, s, p], (r - 1, c, l)
            ), has_prev)

    def part(m, layer):
        return lanes(m * block + layer * half, half)

    def plane_copy(mask, side, s, p, origin, source, device):
        m = member(s, p)
        dst = jr_ref.at[p, m, pl.ds(pl.multiple_of(origin * piece, piece), piece), :]
        return remote(source if source is not None else dst, dst, jr_send.at[mask, side, s, p],
                      jr_recv.at[mask, side, s, p], device)

    def plane_out(s, masks, pairs=range(pair_dev)):
        for mask in masks:
            for p in pairs:
                for side, layer in ((0, l), (1, other)):
                    if mask == 0 and side == 0:
                        continue
                    src = t_ref.at[p, :, part(member(s, p), layer)]
                    send(plane_copy(mask, side, s, p, mine, src, (r, c ^ mask, layer)))

    seen = set()

    def plane_wait(mask, s, p):
        if (mask, s, p) in seen:
            return
        seen.add((mask, s, p))
        for side, layer in ((0, l), (1, other)):
            if mask == 0 and side == 0:
                continue
            plane_copy(mask, side, s, p, (c ^ mask) * 2 + layer, None, partner).wait_recv()

    def plane_relay(s, p, mask):
        plane_wait(mask, s, p)
        for side, layer in ((0, l), (1, other)):
            send(plane_copy(3, side, s, p, (c ^ mask) * 2 + layer, None, (r, c ^ mask ^ 3, l)))

    same = r == c
    differs = r != c

    def other_half(s, p):
        src = jr_ref.at[p, member(s, p)]
        return remote(src, jo_ref.at[p, member(s, p)], jo_send.at[s, p], jo_recv.at[s, p], partner)

    def halves_out(s):
        for p in range(pair_dev):
            send(other_half(s, p), same)

    def arrivals(step):
        for recv, snd, plane, to, into in (
            (zu_recv, zu_send, r - step, r + 1, ju_send),
            (zd_recv, zd_send, r + step, r - 1, jd_send),
        ):
            here = (plane >= 0) & (plane < rows_n)
            onward = here & (to >= 0) & (to < rows_n)
            yield recv, snd, jnp.clip(plane, 0, rows_n - 1), here, onward, to, into

    def hand_over(s, step, among, neighbours=(True, False)):
        for near in neighbours:
            for p in range(pair_dev):
                for _, _, at, here, onward, _, into in arrivals(step):
                    chosen = (onward if among else here & jnp.logical_not(onward)) & (at != c)
                    chosen = chosen & ((at == (c ^ 1)) if near else (at != (c ^ 1)))
                    send(remote(
                        z_ref.at[at, s, p], jc_ref.at[mine, s, p], into.at[step, s, p], jc_recv.at[c ^ at, s, p],
                        (r, at, l),
                    ), chosen)

    def forward(s, step):
        for p in range(pair_dev):
            for recv, snd, at, _, onward, to, _ in arrivals(step):
                block_ref = z_ref.at[at, s, p]
                if step + 1 == rows_n:
                    continue

                @pl.when(onward)
                def _():
                    remote(block_ref, block_ref, snd.at[step, s, p], recv.at[step, s, p], partner).wait_recv()

                send(remote(
                    block_ref, block_ref, snd.at[step, s, p], recv.at[step + 1, s, p], (to, c, l)
                ), onward)

    def finish(s, step):
        for p in range(pair_dev):
            for recv, snd, at, here, onward, _, _ in arrivals(step):
                block_ref = z_ref.at[at, s, p]

                @pl.when(here & jnp.logical_not(onward))
                def _():
                    remote(block_ref, block_ref, snd.at[step, s, p], recv.at[step, s, p], partner).wait_recv()

        hand_over(s, step, False)

    def columns_copy(p):
        rows = pl.ds(p * order, order)
        return remote(a_ref.at[rows], ap_ref.at[rows], ap_send.at[p], ap_recv.at[p], partner)

    def split_columns(src, layer, p):
        count = order // ROWS

        def fetch(at):
            slot = lax.rem(at, 2)
            rows = pl.ds(pl.multiple_of(p * order + at * ROWS, ROWS), ROWS)
            for j in range(width):
                for tile in range(tiles):
                    pltpu.make_async_copy(
                        src.at[rows, tile * width + j, 0, :],
                        a_stage.at[slot, :, pl.ds(j * half + tile * LANES, LANES)],
                        stage_sem.at[slot],
                    ).start()

        def body(at, carry):
            @pl.when(at + 1 < count)
            def _():
                fetch(at + 1)

            slot = lax.rem(at, 2)
            pltpu.make_async_copy(a_stage.at[slot], a_stage.at[slot], stage_sem.at[slot]).wait()
            rows = pl.ds(pl.multiple_of(at * ROWS, ROWS), ROWS)
            for j in range(width):
                high, low = halves_of(a_stage[slot, :, j * half : (j + 1) * half])
                cols = lanes(j * block + layer * half, half)
                a_hi[p, rows, cols] = high
                a_lo[p, rows, cols] = low
            return carry

        fetch(0)
        lax.fori_loop(0, count, body, 0)

    wide = 2 * piece

    def turn(s):
        def fetch(mask):
            for p in range(pair_dev):
                plane_wait(mask, s, p)
            at = pl.ds(pl.multiple_of((c ^ mask) * wide, wide), wide)
            for p in range(pair_dev):
                pltpu.make_async_copy(
                    jr_ref.at[p, member(s, p), at, :], j_stage.at[mask % 2, p], stage_sem.at[mask % 2]
                ).start()

        fetch(0)
        for mask in range(cols_n):
            if mask + 1 < cols_n:
                fetch(mask + 1)
            stage = j_stage.at[mask % 2]
            pltpu.make_async_copy(stage, stage, stage_sem.at[mask % 2]).wait()
            at = lanes((c ^ mask) * wide, wide)
            for p in range(pair_dev):
                high, low = halves_of(j_stage[mask % 2, p].T)
                jt_hi[slot_of(s, p), :, at] = high
                jt_lo[slot_of(s, p), :, at] = low

    def left(slot):
        p = slot // 2

        def body(n, carry):
            cols = lanes(n * block, block)
            l_tile[slot * width + n] = three_dots(
                jt_hi[slot], jt_lo[slot], a_hi[p, :, cols], a_lo[p, :, cols]
            )
            return carry

        lax.fori_loop(0, width, body, 0)

    def left_out(slot, order_of_tiles):
        if slot == 1:
            moved, target, at = has_prev, r - 1, jnp.where(has_prev, 3, 2)
        elif slot == width - 2:
            moved, target, at = has_next, r + 1, jnp.where(has_next, 0, 3)
        else:
            moved, target, at = None, r, (jnp.where(has_prev, 2, 0) if slot == 0 else 1)
        for n in order_of_tiles:
            src, dst = l_tile.at[slot * width + n], lr_ref.at[at, n]
            here = pltpu.make_async_copy(src, dst, lr_recv.at[at, n])
            if moved is None:
                here.start()
            else:
                send(remote(src, dst, lr_send.at[slot, n], lr_recv.at[at, n], (target, c, l)), moved)
                pl.when(jnp.logical_not(moved))(here.start)

    def right_pieces(s):
        masks = list(range(1, cols_n)) + [0]
        deep = c_stage.shape[0]

        def handed(mask, index, src):
            return remote(src, jc_ref.at[index, s], jp_send.at[mask, s], jp_recv.at[mask, s], partner)

        todo = []
        for mask in masks:
            index = (c ^ mask) * 2 + l
            src = jc_ref.at[index, s] if mask else z_ref.at[c, s]
            copy = handed(mask, index, src)
            todo.append((src, index, mask, copy, True))
            pending.append((copy, differs))
        for mask in masks:
            index = (c ^ mask) * 2 + other
            src = jc_ref.at[index, s]
            todo.append((src, index, mask, handed(mask, index, src), False))

        def fetch(n):
            src, _, _, copy, first_hand = todo[n]
            if not first_hand:
                copy.wait_recv()
            load = pltpu.make_async_copy(src, c_stage.at[n % deep], c_sem.at[n % deep])
            load.start()
            return load

        @pl.when(differs)
        def _():
            for src, index, mask, copy, first_hand in todo:
                if first_hand:
                    if mask:
                        for p in range(pair_dev):
                            got = jc_ref.at[index, s, p]
                            remote(got, got, jp_send.at[mask, s], jc_recv.at[mask, s, p], partner).wait_recv()
                    copy.start()
            loads = [fetch(n) for n in range(deep - 1)]
            for n, (_, index, _, _, _) in enumerate(todo):
                if n + deep - 1 < len(todo):
                    loads.append(fetch(n + deep - 1))
                loads[n].wait()
                rows = pl.ds(pl.multiple_of(index * piece, piece), piece)
                for p in range(pair_dev):
                    high, low = halves_of(c_stage[n % deep, p])
                    jc_hi[slot_of(s, p), rows, :] = high
                    jc_lo[slot_of(s, p), rows, :] = low

        @pl.when(same)
        def _():
            jobs = [(side, n) for side in range(2) for n in range(cols_n)]

            def fetch(k):
                side, n = jobs[k]
                if side == 1 and n == 0:
                    for p in range(pair_dev):
                        other_half(s, p).wait_recv()
                for p in range(pair_dev):
                    src = (jo_ref if side else jr_ref).at[p, member(s, p), pl.ds(n * wide, wide), :]
                    pltpu.make_async_copy(src, j_stage.at[k % 2, p], stage_sem.at[k % 2]).start()

            fetch(0)
            for k, (side, n) in enumerate(jobs):
                if k + 1 < len(jobs):
                    fetch(k + 1)
                stage = j_stage.at[k % 2]
                pltpu.make_async_copy(stage, stage, stage_sem.at[k % 2]).wait()
                cols = lanes((other if side else l) * half, half)
                for p in range(pair_dev):
                    high, low = halves_of(j_stage[k % 2, p])
                    jc_hi[slot_of(s, p), n * wide : (n + 1) * wide, cols] = high
                    jc_lo[slot_of(s, p), n * wide : (n + 1) * wide, cols] = low

    def left_rows(at, q):
        loads = []
        for n in (2 * q, 2 * q + 1):
            src = lr_ref.at[at, n]
            pltpu.make_async_copy(src, src, lr_recv.at[at, n]).wait()
            loads.append(pltpu.make_async_copy(src, l_stage.at[n % 2], stage_sem.at[n % 2]))
            loads[-1].start()
        for n in (2 * q, 2 * q + 1):
            loads[n % 2].wait()
            high, low = halves_of(l_stage[n % 2])
            cols = slice(n * block, (n + 1) * block)
            lr_hi[at, :, cols] = high
            lr_lo[at, :, cols] = low

    left_end, right_end = c > 0, c + 1 < cols_n
    staying, arriving = (1, width - 2), (0, width - 1)
    by_way = (staying[0], arriving[0]) if square else ()
    low_rows = pl.ds(pl.multiple_of(l * half, half), half)

    def right(at, j):
        q = j // 2
        rows = slice(q * order, (q + 1) * order)
        tile = at * width + j
        o_tile[tile] = three_dots(lr_hi[at, :, rows], lr_lo[at, :, rows], jc_hi[j], jc_lo[j])
        around = None
        if j == 1:
            moved, target, slot = left_end, c - 1, jnp.where(left_end, 3, 2)
            if at in by_way:
                around = c == 2
        elif j == width - 2:
            moved, target, slot = right_end, c + 1, jnp.where(right_end, 0, 3)
            if at in by_way:
                around = c == 1
        else:
            moved, target, slot = None, c, (jnp.where(left_end, 2, 0) if j == 0 else 1)
        dst = out_ref.at[slot, at, low_rows, :]
        column = c if moved is None else jnp.where(moved, target, c)
        for s, layer in ((0, l), (1, other)):
            src = o_tile.at[tile, :, lanes(layer * half, half)]
            condition = moved if s == 0 else None
            if around is not None:
                index = by_way.index(at)
                send(remote(
                    src, via_ref.at[index, l], o_send.at[tile, s], via_recv.at[index, l], (r, c ^ 2, layer)
                ), around)
                direct = jnp.logical_not(around)
                condition = direct if condition is None else condition & direct
            if s == 1 or moved is not None:
                send(remote(src, dst, o_send.at[tile, s], o_recv.at[slot, l], (r, column, layer)), condition)
            if s == 0:
                here = pltpu.make_async_copy(src, dst, o_recv.at[slot, l])
                if moved is None:
                    here.start()
                else:
                    pl.when(jnp.logical_not(moved))(here.start)

    def right_relay(index):
        outer = (c == 0) | (c == cols_n - 1)
        slot = jnp.where(c == 0, 3, 0)
        for layer in range(2):
            src = via_ref.at[index, layer]
            rows = pl.ds(layer * half, half)

            @pl.when(outer)
            def _():
                remote(src, src, via_send.at[index, layer], via_recv.at[index, layer], partner).wait_recv()

            send(remote(
                src, out_ref.at[slot, by_way[index], rows, :], via_send.at[index, layer], o_recv.at[slot, layer],
                (r, c ^ 1, l),
            ), outer)

    rows_out(0)
    if square:
        plane_out(0, (1, 2, 0))
        plane_out(1, (1, 0))
    else:
        for s in range(2):
            plane_out(s, list(range(1, cols_n)) + [0])
    for p in range(pair_dev):
        send(columns_copy(p))
    load = pltpu.make_async_copy(t_ref, own_v, own_sem.at[0, 0, 0])
    load.start()
    load.wait()
    fills = []
    for s in range(2):
        for p in range(pair_dev):
            m = member(s, p)
            fills.append(pltpu.make_async_copy(
                own_v.at[p, :, pl.ds(m * block, block)], z_ref.at[r, s, p], own_sem.at[0, s, p]
            ))
            fills.append(pltpu.make_async_copy(
                own_v.at[p, :, part(m, l)],
                jr_ref.at[p, m, pl.ds(pl.multiple_of(mine * piece, piece), piece), :], own_sem.at[1, s, p]
            ))
    for copy in fills:
        copy.start()
    with scope("split_own"):
        for p in range(pair_dev):
            split_columns(a_ref, l, p)
    for copy in fills:
        copy.wait()
    if square:
        with scope("relay0"):
            for p in range(pair_dev):
                plane_relay(0, p, 1)
        plane_out(1, (2,), (1, 0))
    with scope("fwd_a1"):
        forward(0, 1)
        hand_over(0, 1, True, (True,))
    with scope("split_p0"):
        columns_copy(0).wait_recv()
        split_columns(ap_ref, other, 0)
    with scope("split_p1"):
        for p in range(1, pair_dev):
            columns_copy(p).wait_recv()
            split_columns(ap_ref, other, p)
    for step in range(2, rows_n - 1):
        with scope("fwd_a2"):
            forward(0, step)
            hand_over(0, step, True, (True,))
    rows_out(1)
    if square:
        with scope("relay1"):
            plane_relay(1, 0, 1)
    for step in range(1, rows_n - 1):
        hand_over(0, step, True, (False,))
    with scope("turn_a"):
        turn(0)
    halves_out(0)
    with scope("left_a2"):
        left(width - 2)
    for step in range(1, rows_n):
        with scope("fin_a"):
            finish(0, step)
    if square:
        with scope("relay2"):
            plane_relay(1, 1, 2)
    with scope("fwd_b1"):
        forward(1, 1)
        hand_over(1, 1, True)
    with scope("left_a1"):
        left(1)
    with scope("turn_b"):
        turn(1)
    halves_out(1)
    for step in range(2, rows_n - 1):
        with scope("fwd_b2"):
            forward(1, step)
            hand_over(1, step, True)
    first, last = (0, 1), (2, 3)
    for tiles_first, tiles_last in ((first, last), (last, first)):
        left_out(width - 2, tiles_first)
        left_out(1, tiles_last)
    with scope("left_b"):
        for slot in (0, width - 1):
            left(slot)
            left_out(slot, range(width))
    for at in staying:
        with scope("rows"):
            for q in range(pair_dev):
                left_rows(at, q)
    for step in range(1, rows_n):
        with scope("fin_b"):
            finish(1, step)
    with scope("pieces_a"):
        right_pieces(0)
    moving = (1, width - 2)
    for at in staying:
        with scope("right"):
            for j in moving:
                right(at, j)
    for at, q in ((0, 0), (width - 1, 1)):
        with scope("rows_arr"):
            left_rows(at, q)
        with scope("right"):
            right(at, moving[q])
    with scope("pieces_b"):
        right_pieces(1)
    if square:
        with scope("via0"):
            right_relay(0)
    for at, q in ((0, 1), (width - 1, 0)):
        with scope("rows_arr"):
            left_rows(at, q)
        with scope("right"):
            right(at, moving[q])
    with scope("right_local"):
        for at in staying:
            for j in (0, width - 1):
                right(at, j)
    if square:
        with scope("via1"):
            right_relay(1)
    with scope("right_local"):
        for at in arriving:
            for j in (0, width - 1):
                right(at, j)

    with scope("out_wait"):
        for slot in range(width):
            for layer in range(2):
                block_ref = out_ref.at[slot, :, pl.ds(layer * half, half), :]
                pltpu.make_async_copy(block_ref, block_ref, o_recv.at[slot, layer]).wait()
    with scope("send_wait"):
        for copy, condition in pending:
            if condition is None:
                copy.wait_send()
            else:
                pl.when(condition)(copy.wait_send)


def spread(size, x_ref, o_ref, buffer, in_sem, out_sem):
    width, block, tiles = size
    rows = buffer.shape[2]
    steps = block // rows

    def inward(k):
        i, at = k // steps, k % steps
        return pltpu.make_async_copy(x_ref.at[:, i, pl.ds(at * rows, rows), :], buffer.at[k], in_sem.at[k])

    def outward(k, j, tile):
        return pltpu.make_async_copy(
            buffer.at[k, j, :, pl.ds(tile * LANES, LANES)],
            o_ref.at[pl.ds(k * rows, rows), tile * width + j, 0, :], out_sem.at[k, j, tile],
        )

    every = range(width * steps)
    for k in every:
        inward(k).start()
    for k in every:
        inward(k).wait()
        for j in range(width):
            for tile in range(tiles):
                outward(k, j, tile).start()
    for k in every:
        for j in range(width):
            for tile in range(tiles):
                outward(k, j, tile).wait()


def shards(matrix, transforms):
    width, block, _, half = matrix.shape
    pair_dev = width // 2
    order = 2 * block
    rows_n, cols_n = lax.axis_size("row"), lax.axis_size("col")
    tiles = half // LANES
    raw_shape = (width * block, width * tiles, 1, LANES)
    own = transforms[0]
    piece = own.shape[1]
    pieces = 2 * cols_n
    f32, bf16 = jnp.float32, jnp.bfloat16

    raw = matrix.reshape(width * block, width, tiles, LANES).transpose(0, 2, 1, 3).reshape(raw_shape)
    any_space = pl.BlockSpec(memory_space=pl.ANY)
    dma = pltpu.SemaphoreType.DMA
    vmem = pltpu.VMEM
    by_piece = (2, pair_dev)
    flops = 3 * 2 * 2 * width * half * order * width * block
    outs = pl.pallas_call(
        functools.partial(sweep, (rows_n, cols_n, pair_dev, width, block, half, piece)),
        name="sweep",
        out_shape=[
            jax.ShapeDtypeStruct((width, width, block, half), f32),
            jax.ShapeDtypeStruct(raw_shape, f32),
            jax.ShapeDtypeStruct((pair_dev, 2, order, half), f32),
            jax.ShapeDtypeStruct((pair_dev, 2, order, half), f32),
            jax.ShapeDtypeStruct((rows_n, 2, pair_dev, piece, block), f32),
            jax.ShapeDtypeStruct((pieces, 2, pair_dev, piece, block), f32),
            jax.ShapeDtypeStruct((width, width, half, block), f32),
            jax.ShapeDtypeStruct((2, 2, half, half), f32),
        ],
        in_specs=[any_space, any_space],
        out_specs=[any_space] * 8,
        scratch_shapes=[
            vmem((pair_dev, order, width * block), bf16),
            vmem((pair_dev, order, width * block), bf16),
            vmem((width, half, order), bf16),
            vmem((width, half, order), bf16),
            vmem((width, order, block), bf16),
            vmem((width, order, block), bf16),
            vmem((width, half, width * block), bf16),
            vmem((width, half, width * block), bf16),
            vmem((width * width, half, block), f32),
            vmem((width * width, half, block), f32),
            vmem((pair_dev, piece, order), f32),
            vmem((2, ROWS, width * half), f32),
            vmem((2, pair_dev, 2 * piece, half), f32),
            vmem((4, pair_dev, piece, block), f32),
            vmem((2, half, block), f32),
            dma((2,)), dma((4,)), dma((2,) + by_piece),
            dma((pair_dev,)), dma((pair_dev,)),
            dma((cols_n, 2) + by_piece), dma((cols_n, 2) + by_piece),
            dma((rows_n,) + by_piece), dma((rows_n,) + by_piece), dma((rows_n,) + by_piece), dma((rows_n,) + by_piece),
            dma((rows_n,) + by_piece), dma((rows_n,) + by_piece), dma((cols_n,) + by_piece),
            dma((cols_n, 2)), dma((cols_n, 2)), dma(by_piece), dma(by_piece),
            dma((width, width)), dma((width, width)),
            dma((width * width, 2)), dma((width, 2)),
            dma((2, 2)), dma((2, 2)),
        ],
        compiler_params=pltpu.CompilerParams(
            collective_id=0, has_side_effects=True, vmem_limit_bytes=VMEM_LIMIT
        ),
        cost_estimate=pl.CostEstimate(flops=flops, bytes_accessed=0, transcendentals=0),
    )(raw, own)
    blocks = outs[0]

    steps = width * block // ROWS
    result = pl.pallas_call(
        functools.partial(spread, (width, block, tiles)),
        name="spread",
        in_specs=[any_space],
        out_specs=any_space,
        out_shape=jax.ShapeDtypeStruct(raw_shape, f32),
        scratch_shapes=[
            vmem((steps, width, ROWS, half), f32), dma((steps,)), dma((steps, width, tiles)),
        ],
    )(blocks)
    result = result.reshape(width, block, tiles, width, LANES).transpose(0, 1, 3, 2, 4)
    return result.reshape(width, block, width, half)


def solution(mesh):
    return jax.shard_map(
        shards,
        mesh=mesh,
        in_specs=(P("row", None, "col", "layer"), P(None, "row", ("col", "layer"), None)),
        out_specs=P("row", None, "col", "layer"),
        check_vma=False,
    )
```

```python
import functools

import jax
import jax.numpy as jnp
from jax import lax
from jax.experimental import pallas as pl
from jax.experimental.pallas import tpu as pltpu
from jax.sharding import PartitionSpec as P

MESH = pl.DeviceIdType.MESH
LANES = 128
ROWS = 256
VMEM_LIMIT = 66_000_000
scope = jax.named_scope


def halves_of(x):
    high = x.astype(jnp.bfloat16)
    low = (x - high.astype(jnp.float32)).astype(jnp.bfloat16)
    return high, low


def three_dots(a_high, a_low, b_high, b_low):
    def dot(a, b):
        return lax.dot_general(a, b, (((1,), (0,)), ((), ())), preferred_element_type=jnp.float32)

    return dot(a_high, b_high) + (dot(a_high, b_low) + dot(a_low, b_high))


def sweep(
    size,
    a_ref, t_ref,
    out_ref, ap_ref, jr_ref, jo_ref, z_ref, lr_ref, via_ref,
    a_hi, a_lo, jt_hi, jt_lo, jc_hi, jc_lo, lr_hi, lr_lo, l_tile, o_tile,
    own_v, a_stage, j_stage, l_stage,
    stage_sem, j_sem, own_sem,
    ap_send, ap_recv, jr_send, jr_recv,
    zo_send, zu_send, zu_recv, zd_send, zd_recv,
    ju_send, jd_send, jc_recv, jo_send, jo_recv,
    lr_send, lr_recv, o_send, o_recv, via_send, via_recv,
):
    rows_n, cols_n, pair_dev, width, block, half, piece = size
    order = 2 * block
    tiles = half // LANES
    r = lax.axis_index("row")
    c = lax.axis_index("col")
    l = lax.axis_index("layer")
    other = 1 - l
    partner = (r, c, other)
    mine = c * 2 + l
    square = cols_n == 4
    pending = []

    def remote(src, dst, send, recv, device):
        return pltpu.make_async_remote_copy(
            src_ref=src, dst_ref=dst, send_sem=send, recv_sem=recv, device_id=device, device_id_type=MESH
        )

    def send(copy, condition=None):
        if condition is None:
            copy.start()
        else:
            pl.when(condition)(copy.start)
        pending.append((copy, condition))

    def lanes(start, count):
        return pl.ds(pl.multiple_of(start, LANES), count)

    def member(s, p):
        return 1 - p if s == 0 else p

    def slot_of(s, p):
        return 2 * p + member(s, p)

    barrier = pltpu.get_barrier_semaphore()
    for mask in range(cols_n):
        for layer in (l, other):
            if mask == 0 and layer is l:
                continue
            pl.semaphore_signal(barrier, inc=1, device_id=(r, c ^ mask, layer), device_id_type=MESH)
    has_next = r + 1 < rows_n
    has_prev = r > 0

    for layer in (l, other):
        @pl.when(has_next)
        def _():
            pl.semaphore_signal(barrier, inc=1, device_id=(r + 1, c, layer), device_id_type=MESH)

        @pl.when(has_prev)
        def _():
            pl.semaphore_signal(barrier, inc=1, device_id=(r - 1, c, layer), device_id_type=MESH)

    with scope("barrier"):
        pl.semaphore_wait(barrier, 2 * (cols_n + has_next.astype(jnp.int32) + has_prev.astype(jnp.int32)) - 1)

    def part(m, layer):
        return lanes(m * block + layer * half, half)

    def plane_copy(mask, side, s, p, origin, source, device):
        m = member(s, p)
        dst = jr_ref.at[p, m, pl.ds(pl.multiple_of(origin * piece, piece), piece), :]
        return remote(source if source is not None else dst, dst, jr_send.at[mask, side, s, p],
                      jr_recv.at[mask, side, s, p], device)

    def plane_out(s, masks, pairs=range(pair_dev)):
        for mask in masks:
            for p in pairs:
                for side, layer in ((0, l), (1, other)):
                    if mask == 0 and side == 0:
                        continue
                    src = t_ref.at[p, :, part(member(s, p), layer)]
                    send(plane_copy(mask, side, s, p, mine, src, (r, c ^ mask, layer)))

    seen = set()

    def plane_wait(mask, s, p):
        if (mask, s, p) in seen:
            return
        seen.add((mask, s, p))
        for side, layer in ((0, l), (1, other)):
            if mask == 0 and side == 0:
                continue
            plane_copy(mask, side, s, p, (c ^ mask) * 2 + layer, None, partner).wait_recv()

    def plane_relay(s, p, mask):
        plane_wait(mask, s, p)
        for side, layer in ((0, l), (1, other)):
            send(plane_copy(3, side, s, p, (c ^ mask) * 2 + layer, None, (r, c ^ mask ^ 3, l)))

    same = r == c
    differs = r != c
    wide = 2 * piece

    def chip_rows(column):
        return pl.ds(pl.multiple_of(column * wide, wide), wide)

    def left_unit(mask, s, p):
        return jr_ref.at[p, member(s, p), chip_rows(c ^ mask), :]

    def handed(mask, s, p, src):
        return remote(
            src, jo_ref.at[mask, s, p], jo_send.at[mask, s, p], jo_recv.at[mask, s, p], partner
        )

    def halves_out(s):
        for mask in range(cols_n):
            for p in range(pair_dev):
                send(handed(mask, s, p, left_unit(mask, s, p)), same)

    kinds = (0, 1) if square else (0,)

    def carried(kind, s, group, up):
        if not square:
            return True
        side = ((c ^ group) & 1) == 0
        if s == 1:
            return side
        crossed = (group == 1) if up else (group == rows_n - 2)
        return crossed & side if kind else jnp.logical_not(crossed) | side

    def ways():
        return (
            (True, has_next, r + 1, zu_send, zu_recv), (False, has_prev, r - 1, zd_send, zd_recv)
        )

    def rows_out(s):
        for p in range(pair_dev):
            for side, layer in ((0, l), (1, other)):
                for up, there, to, _, recv in ways():
                    send(remote(
                        t_ref.at[p, :, part(member(s, p), layer)],
                        z_ref.at[r, 0, s, p, pl.ds(pl.multiple_of(l * piece, piece), piece), :],
                        zo_send.at[int(up), side, s, p], recv.at[1, 0, s, p], (to, c, layer),
                    ), there & carried(0, s, r, up))

    def rows_across(s):
        for p in range(pair_dev):
            plane_wait(1, s, p)
            for up, there, to, snd, recv in ways():
                send(remote(
                    left_unit(1, s, p), z_ref.at[r, 1, s, p], snd.at[0, 1, s, p], recv.at[1, 1, s, p], (to, c, l)
                ), there & carried(1, s, r, up))

    def arrivals(s, step):
        for kind in kinds:
            for up, recv, snd, plane, to, into in (
                (True, zu_recv, zu_send, r - step, r + 1, ju_send),
                (False, zd_recv, zd_send, r + step, r - 1, jd_send),
            ):
                at = jnp.clip(plane, 0, rows_n - 1)
                here = (plane >= 0) & (plane < rows_n) & carried(kind, s, at, up)
                onward = here & (to >= 0) & (to < rows_n)
                yield kind, recv, snd, at, here, onward, to, into

    def hand_over(s, step, among, only=None, ends=None):
        for p in range(pair_dev):
            for kind, _, _, at, here, onward, _, into in arrivals(s, step):
                if only not in (None, kind):
                    continue
                chosen = (onward if among else here & jnp.logical_not(onward)) & (at != c)
                if ends is not None:
                    at_end = (at == 0) | (at == rows_n - 1)
                    chosen = chosen & (at_end if ends else jnp.logical_not(at_end))
                mask = (c ^ at) ^ kind
                send(remote(
                    z_ref.at[at, kind, s, p], z_ref.at[at, mask, s, p], into.at[step, kind, s, p],
                    jc_recv.at[mask, s, p], (r, at, l),
                ), chosen)

    def forward(s, step, give=True, only=None, ends=None):
        for p in range(pair_dev):
            for kind, recv, snd, at, _, onward, to, _ in arrivals(s, step):
                block_ref = z_ref.at[at, kind, s, p]
                if step + 1 == rows_n or only not in (None, kind):
                    continue
                if ends is not None:
                    at_end = (at == 0) | (at == rows_n - 1)
                    onward = onward & (at_end if ends else jnp.logical_not(at_end))

                @pl.when(onward)
                def _():
                    remote(block_ref, block_ref, snd.at[step, kind, s, p], recv.at[step, kind, s, p],
                           partner).wait_recv()

                send(remote(
                    block_ref, block_ref, snd.at[step, kind, s, p], recv.at[step + 1, kind, s, p], (to, c, l)
                ), onward)
        if give:
            hand_over(s, step, True, only, ends)

    def finish(s, step):
        for p in range(pair_dev):
            for kind, recv, snd, at, here, onward, _, _ in arrivals(s, step):
                block_ref = z_ref.at[at, kind, s, p]

                @pl.when(here & jnp.logical_not(onward))
                def _():
                    remote(block_ref, block_ref, snd.at[step, kind, s, p], recv.at[step, kind, s, p],
                           partner).wait_recv()

        hand_over(s, step, False)

    def columns_copy(p):
        rows = pl.ds(p * order, order)
        return remote(a_ref.at[rows], ap_ref.at[rows], ap_send.at[p], ap_recv.at[p], partner)

    def split_columns(src, layer, p):
        count = order // ROWS

        def fetch(at):
            slot = lax.rem(at, 2)
            rows = pl.ds(pl.multiple_of(p * order + at * ROWS, ROWS), ROWS)
            for j in range(width):
                for tile in range(tiles):
                    pltpu.make_async_copy(
                        src.at[rows, tile * width + j, 0, :],
                        a_stage.at[slot, :, pl.ds(j * half + tile * LANES, LANES)],
                        stage_sem.at[slot],
                    ).start()

        def body(at, carry):
            @pl.when(at + 1 < count)
            def _():
                fetch(at + 1)

            slot = lax.rem(at, 2)
            pltpu.make_async_copy(a_stage.at[slot], a_stage.at[slot], stage_sem.at[slot]).wait()
            rows = pl.ds(pl.multiple_of(at * ROWS, ROWS), ROWS)
            for j in range(width):
                high, low = halves_of(a_stage[slot, :, j * half : (j + 1) * half])
                cols = lanes(j * block + layer * half, half)
                a_hi[p, rows, cols] = high
                a_lo[p, rows, cols] = low
            return carry

        fetch(0)
        lax.fori_loop(0, count, body, 0)

    def turn(s):
        def fetch(mask):
            for p in range(pair_dev):
                plane_wait(mask, s, p)
            for p in range(pair_dev):
                pltpu.make_async_copy(left_unit(mask, s, p), j_stage.at[mask % 2, p], j_sem.at[mask % 2]).start()

        fetch(0)
        for mask in range(cols_n):
            if mask + 1 < cols_n:
                fetch(mask + 1)
            stage = j_stage.at[mask % 2]
            pltpu.make_async_copy(stage, stage, j_sem.at[mask % 2]).wait()
            at = lanes((c ^ mask) * wide, wide)
            for p in range(pair_dev):
                high, low = halves_of(j_stage[mask % 2, p].T)
                jt_hi[slot_of(s, p), :, at] = high
                jt_lo[slot_of(s, p), :, at] = low
        halves_out(s)

    def left(slot):
        p = slot // 2
        kept = slot in (0, width - 1)
        at = (jnp.where(has_prev, 2, 0) if slot == 0 else 1) if kept else None

        def body(n, carry):
            cols = lanes(n * block, block)
            x = three_dots(jt_hi[slot], jt_lo[slot], a_hi[p, :, cols], a_lo[p, :, cols])
            if kept:
                high, low = halves_of(x)
                lr_hi[at, :, cols] = high
                lr_lo[at, :, cols] = low
            else:
                l_tile[(slot - 1) * width + n] = x
            return carry

        lax.fori_loop(0, width, body, 0)

    def left_out(slot, order_of_tiles):
        if slot == 1:
            moved, target, at = has_prev, r - 1, jnp.where(has_prev, 3, 2)
        else:
            moved, target, at = has_next, r + 1, jnp.where(has_next, 0, 3)
        for n in order_of_tiles:
            src, dst = l_tile.at[(slot - 1) * width + n], lr_ref.at[at, n]
            send(remote(src, dst, lr_send.at[slot, n], lr_recv.at[at, n], (target, c, l)), moved)
            pl.when(jnp.logical_not(moved))(pltpu.make_async_copy(src, dst, lr_recv.at[at, n]).start)

    def right_pieces(s):
        deep = j_stage.shape[0]
        for mask in range(cols_n):
            for p in range(pair_dev):
                unit = z_ref.at[c, mask, s, p]
                late = differs
                if square and mask == 1:
                    late = differs & jnp.logical_not(jnp.where(r > c, c == 1, c == rows_n - 2))
                if mask and not (square and mask == 1 and s == 1):
                    @pl.when(late)
                    def _():
                        remote(unit, unit, jo_send.at[mask, s, p], jc_recv.at[mask, s, p], partner).wait_recv()

                send(handed(mask, s, p, unit), differs)
        jobs = [(side, mask) for side in range(2) for mask in range(cols_n)]

        def fetch(k):
            side, mask = jobs[k]
            for p in range(pair_dev):
                def take(src):
                    return pltpu.make_async_copy(src, j_stage.at[k % deep, p], j_sem.at[k % deep])

                if side:
                    src = jo_ref.at[mask, s, p]
                    handed(mask, s, p, src).wait_recv()
                    take(src).start()
                else:
                    pl.when(differs)(take(z_ref.at[c, mask, s, p]).start)
                    pl.when(same)(take(left_unit(mask, s, p)).start)

        for k in range(deep - 1):
            fetch(k)
        for k, (side, mask) in enumerate(jobs):
            if k + deep - 1 < len(jobs):
                fetch(k + deep - 1)
            stage = j_stage.at[k % deep]
            pltpu.make_async_copy(stage, stage, j_sem.at[k % deep]).wait()
            cols = lanes((other if side else l) * half, half)
            for p in range(pair_dev):
                high, low = halves_of(j_stage[k % deep, p])
                jc_hi[slot_of(s, p), chip_rows(c ^ mask), cols] = high
                jc_lo[slot_of(s, p), chip_rows(c ^ mask), cols] = low

    def left_rows(at, q):
        loads = []
        for n in range(2):
            src = lr_ref.at[at, 2 * q + n]
            pltpu.make_async_copy(src, src, lr_recv.at[at, 2 * q + n]).wait()
            loads.append(pltpu.make_async_copy(src, l_stage.at[n], stage_sem.at[n]))
            loads[-1].start()
        for n in range(2):
            loads[n].wait()
            high, low = halves_of(l_stage[n])
            cols = lanes((2 * q + n) * block, block)
            lr_hi[at, :, cols] = high
            lr_lo[at, :, cols] = low

    left_end, right_end = c > 0, c + 1 < cols_n
    staying, arriving = (1, width - 2), (0, width - 1)
    by_way = staying if square else ()
    low_rows = pl.ds(pl.multiple_of(l * half, half), half)

    def right_tile(at, j, q):
        rows = lanes(q * order, order)
        tile = at * width + j
        o_tile[tile] = three_dots(lr_hi[at, :, rows], lr_lo[at, :, rows], jc_hi[j], jc_lo[j])
        return tile

    def right_moving(at, q):
        j = 1 + q
        tile = right_tile(at, j, q)
        up = q == 1
        moved = jnp.where(up, right_end, left_end)
        target = jnp.where(up, c + 1, c - 1)
        slot = jnp.where(up, jnp.where(right_end, 0, 3), jnp.where(left_end, 3, 2))
        column = jnp.where(moved, target, c)
        dst = out_ref.at[slot, at, low_rows, :]
        around = None
        if isinstance(at, int) and at in by_way:
            around = jnp.where(up, c == 1, c == 2)
        for s, layer in ((0, l), (1, other)):
            src = o_tile.at[tile, :, lanes(layer * half, half)]
            condition = moved if s == 0 else None
            if around is not None:
                index = by_way.index(at)
                send(remote(
                    src, via_ref.at[index, l], o_send.at[tile, s], via_recv.at[index, l], (r, c ^ 2, layer)
                ), around)
                direct = jnp.logical_not(around)
                condition = direct if condition is None else condition & direct
            send(remote(src, dst, o_send.at[tile, s], o_recv.at[slot, l], (r, column, layer)), condition)
            if s == 0:
                pl.when(jnp.logical_not(moved))(pltpu.make_async_copy(src, dst, o_recv.at[slot, l]).start)

    def right_kept(at, j):
        tile = right_tile(at, j, j // 2)
        slot = jnp.where(left_end, 2, 0) if j == 0 else 1
        dst = out_ref.at[slot, at, low_rows, :]
        send(remote(
            o_tile.at[tile, :, lanes(other * half, half)], dst, o_send.at[tile, 1], o_recv.at[slot, l], partner
        ))
        pltpu.make_async_copy(
            o_tile.at[tile, :, lanes(l * half, half)], dst, o_recv.at[slot, l]
        ).start()

    def right_relay(index):
        outer = (c == 0) | (c == cols_n - 1)
        slot = jnp.where(c == 0, 3, 0)
        for layer in range(2):
            src = via_ref.at[index, layer]
            rows = pl.ds(layer * half, half)

            @pl.when(outer)
            def _():
                remote(src, src, via_send.at[index, layer], via_recv.at[index, layer], partner).wait_recv()

            send(remote(
                src, out_ref.at[slot, by_way[index], rows, :], via_send.at[index, layer], o_recv.at[slot, layer],
                (r, c ^ 1, l),
            ), outer)

    rows_out(0)
    if square:
        plane_out(0, (1, 2, 0))
        plane_out(1, (1, 0))
    else:
        for s in range(2):
            plane_out(s, list(range(1, cols_n)) + [0])
    for p in range(pair_dev):
        send(columns_copy(p))
    load = pltpu.make_async_copy(t_ref, own_v, own_sem.at[0, 0, 0])
    load.start()
    load.wait()
    fills = []
    for s in range(2):
        for p in range(pair_dev):
            fills.append(pltpu.make_async_copy(
                own_v.at[p, :, part(member(s, p), l)],
                jr_ref.at[p, member(s, p), pl.ds(pl.multiple_of(mine * piece, piece), piece), :],
                own_sem.at[1, s, p],
            ))
    for copy in fills:
        copy.start()
    with scope("split_own"):
        for p in range(pair_dev):
            split_columns(a_ref, l, p)
    for copy in fills:
        copy.wait()
    if square:
        with scope("relay0"):
            for p in range(pair_dev):
                plane_relay(0, p, 1)
        plane_out(1, (2,))
        rows_across(0)
    with scope("fwd_a1"):
        forward(0, 1, only=0)
    rows_out(1)
    with scope("split_p0"):
        columns_copy(0).wait_recv()
        split_columns(ap_ref, other, 0)
    with scope("split_p1"):
        for p in range(1, pair_dev):
            columns_copy(p).wait_recv()
            split_columns(ap_ref, other, p)
    if square:
        with scope("fwd_a1x"):
            forward(0, 1, only=1)
        with scope("across1"):
            rows_across(1)
    with scope("fwd_b1e0"):
        forward(1, 1, only=0, ends=True)
    with scope("turn_a"):
        turn(0)
    with scope("left_a2"):
        left(width - 2)
    for step in range(2, rows_n - 1):
        with scope("fwd_a2"):
            forward(0, step, False)
    if square:
        with scope("fwd_b1e"):
            forward(1, 1, only=1, ends=True)
    with scope("left_a1"):
        left(1)
    if square:
        with scope("relay1"):
            for p in range(pair_dev):
                plane_relay(1, p, 2)
    for step in range(2, rows_n - 1):
        hand_over(0, step, True)
    for step in range(1, rows_n):
        with scope("fin_a"):
            finish(0, step)
    for step in range(2, rows_n - 1):
        with scope("fwd_b2"):
            forward(1, step)
    with scope("turn_b"):
        turn(1)
    with scope("left_b"):
        for slot in (0, width - 1):
            left(slot)
    with scope("fwd_b1m"):
        forward(1, 1, ends=False)
    first, last = (0, 1), (2, 3)
    for tiles_first, tiles_last in ((first, last), (last, first)):
        left_out(width - 2, tiles_first)
        left_out(1, tiles_last)
    with scope("rows"):
        @pl.when(jnp.logical_not(has_prev))
        def _():
            for q in range(pair_dev):
                left_rows(2, q)
    with scope("pieces_a"):
        right_pieces(0)
    for at in staying:
        with scope("right"):
            for q in range(pair_dev):
                right_moving(at, q)

    first, last = jnp.logical_not(has_prev), jnp.logical_not(has_next)

    def arrived(at, q):
        with scope("rows_arr"):
            @pl.when(has_prev | (at == width - 1))
            def _():
                left_rows(at, q)
        with scope("right"):
            right_moving(at, q)

    top, low = 0, width - 1
    arrived(jnp.where(last, low, top), jnp.where(last, 1, 0))
    arrived(jnp.where(first, top, low), jnp.where(last, 0, 1))
    for step in range(1, rows_n):
        with scope("fin_b"):
            finish(1, step)
    if square:
        with scope("via0"):
            right_relay(0)
            right_relay(1)
    arrived(jnp.where(first, low, top), jnp.where(last, 0, 1))
    arrived(jnp.where(last, top, low), jnp.where(last, 1, 0))
    with scope("pieces_b"):
        right_pieces(1)
    with scope("right_local"):
        for at in staying + arriving:
            for j in (0, width - 1):
                right_kept(at, j)

    with scope("out_wait"):
        for slot in range(width):
            for layer in range(2):
                block_ref = out_ref.at[slot, :, pl.ds(layer * half, half), :]
                pltpu.make_async_copy(block_ref, block_ref, o_recv.at[slot, layer]).wait()
    with scope("send_wait"):
        for copy, condition in pending:
            if condition is None:
                copy.wait_send()
            else:
                pl.when(condition)(copy.wait_send)


def spread(size, x_ref, o_ref, buffer, in_sem, out_sem):
    width, block, tiles = size
    rows = buffer.shape[2]
    steps = block // rows

    def inward(k):
        i, at = k // steps, k % steps
        return pltpu.make_async_copy(x_ref.at[:, i, pl.ds(at * rows, rows), :], buffer.at[k], in_sem.at[k])

    def outward(k, j, tile):
        return pltpu.make_async_copy(
            buffer.at[k, j, :, pl.ds(tile * LANES, LANES)],
            o_ref.at[pl.ds(k * rows, rows), tile * width + j, 0, :], out_sem.at[k, j, tile],
        )

    every = range(width * steps)
    for k in every:
        inward(k).start()
    for k in every:
        inward(k).wait()
        for j in range(width):
            for tile in range(tiles):
                outward(k, j, tile).start()
    for k in every:
        for j in range(width):
            for tile in range(tiles):
                outward(k, j, tile).wait()


def shards(matrix, transforms):
    width, block, _, half = matrix.shape
    pair_dev = width // 2
    order = 2 * block
    rows_n, cols_n = lax.axis_size("row"), lax.axis_size("col")
    tiles = half // LANES
    raw_shape = (width * block, width * tiles, 1, LANES)
    own = transforms[0]
    piece = own.shape[1]
    f32, bf16 = jnp.float32, jnp.bfloat16

    raw = matrix.reshape(width * block, width, tiles, LANES).transpose(0, 2, 1, 3).reshape(raw_shape)
    any_space = pl.BlockSpec(memory_space=pl.ANY)
    dma = pltpu.SemaphoreType.DMA
    vmem = pltpu.VMEM
    by_piece = (2, pair_dev)
    by_unit = by_piece + (2 * piece, half)
    flops = 3 * 2 * 2 * width * half * order * width * block
    outs = pl.pallas_call(
        functools.partial(sweep, (rows_n, cols_n, pair_dev, width, block, half, piece)),
        name="sweep",
        out_shape=[
            jax.ShapeDtypeStruct((width, width, block, half), f32),
            jax.ShapeDtypeStruct(raw_shape, f32),
            jax.ShapeDtypeStruct((pair_dev, 2, order, half), f32),
            jax.ShapeDtypeStruct((cols_n,) + by_unit, f32),
            jax.ShapeDtypeStruct((rows_n, cols_n) + by_unit, f32),
            jax.ShapeDtypeStruct((width, width, half, block), f32),
            jax.ShapeDtypeStruct((2, 2, half, half), f32),
        ],
        in_specs=[any_space, any_space],
        out_specs=[any_space] * 7,
        scratch_shapes=[
            vmem((pair_dev, order, width * block), bf16),
            vmem((pair_dev, order, width * block), bf16),
            vmem((width, half, order), bf16),
            vmem((width, half, order), bf16),
            vmem((width, order, block), bf16),
            vmem((width, order, block), bf16),
            vmem((width, half, width * block), bf16),
            vmem((width, half, width * block), bf16),
            vmem((2 * width, half, block), f32),
            vmem((width * width, half, block), f32),
            vmem((pair_dev, piece, order), f32),
            vmem((2, ROWS, width * half), f32),
            vmem((4, pair_dev, 2 * piece, half), f32),
            vmem((2, half, block), f32),
            dma((2,)), dma((4,)), dma((2,) + by_piece),
            dma((pair_dev,)), dma((pair_dev,)),
            dma((cols_n, 2) + by_piece), dma((cols_n, 2) + by_piece),
            dma((2, 2) + by_piece),
            dma((rows_n, 2) + by_piece), dma((rows_n, 2) + by_piece),
            dma((rows_n, 2) + by_piece), dma((rows_n, 2) + by_piece),
            dma((rows_n, 2) + by_piece), dma((rows_n, 2) + by_piece), dma((cols_n,) + by_piece),
            dma((cols_n,) + by_piece), dma((cols_n,) + by_piece),
            dma((width, width)), dma((width, width)),
            dma((width * width, 2)), dma((width, 2)),
            dma((2, 2)), dma((2, 2)),
        ],
        compiler_params=pltpu.CompilerParams(
            collective_id=0, has_side_effects=True, vmem_limit_bytes=VMEM_LIMIT
        ),
        cost_estimate=pl.CostEstimate(flops=flops, bytes_accessed=0, transcendentals=0),
    )(raw, own)
    blocks = outs[0]

    steps = width * block // ROWS
    result = pl.pallas_call(
        functools.partial(spread, (width, block, tiles)),
        name="spread",
        in_specs=[any_space],
        out_specs=any_space,
        out_shape=jax.ShapeDtypeStruct(raw_shape, f32),
        scratch_shapes=[
            vmem((steps, width, ROWS, half), f32), dma((steps,)), dma((steps, width, tiles)),
        ],
    )(blocks)
    result = result.reshape(width, block, tiles, width, LANES).transpose(0, 1, 3, 2, 4)
    return result.reshape(width, block, width, half)


def solution(mesh):
    return jax.shard_map(
        shards,
        mesh=mesh,
        in_specs=(P("row", None, "col", "layer"), P(None, "row", ("col", "layer"), None)),
        out_specs=P("row", None, "col", "layer"),
        check_vma=False,
    )
```

```python
import functools

import jax
import jax.numpy as jnp
from jax import lax
from jax.experimental import pallas as pl
from jax.experimental.pallas import tpu as pltpu
from jax.sharding import PartitionSpec as P

MESH = pl.DeviceIdType.MESH
LANES = 128
ROWS = 256
VMEM_LIMIT = 66_000_000
scope = jax.named_scope


def halves_of(x):
    high = x.astype(jnp.bfloat16)
    low = (x - high.astype(jnp.float32)).astype(jnp.bfloat16)
    return high, low


def three_dots(a_high, a_low, b_high, b_low):
    def dot(a, b):
        return lax.dot_general(a, b, (((1,), (0,)), ((), ())), preferred_element_type=jnp.float32)

    return dot(a_high, b_high) + (dot(a_high, b_low) + dot(a_low, b_high))


def sweep(
    size,
    a_ref, t_ref,
    out_ref, ap_ref, jr_ref, jo_ref, z_ref, lr_ref, via_ref,
    a_hi, a_lo, jt_hi, jt_lo, jc_hi, jc_lo, lr_hi, lr_lo, l_tile, o_tile,
    own_v, a_stage, j_stage, l_stage,
    stage_sem, j_sem, own_sem,
    ap_send, ap_recv, jr_send, jr_recv,
    zo_send, zu_send, zu_recv, zd_send, zd_recv,
    ju_send, jd_send, jc_recv, jo_send, jo_recv,
    lr_send, lr_recv, o_send, o_recv, via_send, via_recv,
):
    rows_n, cols_n, pair_dev, width, block, half, piece = size
    order = 2 * block
    tiles = half // LANES
    r = lax.axis_index("row")
    c = lax.axis_index("col")
    l = lax.axis_index("layer")
    other = 1 - l
    partner = (r, c, other)
    mine = c * 2 + l
    square = cols_n == 4
    pending = []

    def remote(src, dst, send, recv, device):
        return pltpu.make_async_remote_copy(
            src_ref=src, dst_ref=dst, send_sem=send, recv_sem=recv, device_id=device, device_id_type=MESH
        )

    def send(copy, condition=None):
        if condition is None:
            copy.start()
        else:
            pl.when(condition)(copy.start)
        pending.append((copy, condition))

    def lanes(start, count):
        return pl.ds(pl.multiple_of(start, LANES), count)

    def member(s, p):
        return 1 - p if s == 0 else p

    def leading(group, k):
        return jnp.where((group & 1) == 0 if square else group == 0, 1 - k, k)

    def slot_of(s, p):
        return 2 * p + member(s, p)

    barrier = pltpu.get_barrier_semaphore()
    for mask in range(cols_n):
        for layer in (l, other):
            if mask == 0 and layer is l:
                continue
            pl.semaphore_signal(barrier, inc=1, device_id=(r, c ^ mask, layer), device_id_type=MESH)
    has_next = r + 1 < rows_n
    has_prev = r > 0

    for layer in (l, other):
        @pl.when(has_next)
        def _():
            pl.semaphore_signal(barrier, inc=1, device_id=(r + 1, c, layer), device_id_type=MESH)

        @pl.when(has_prev)
        def _():
            pl.semaphore_signal(barrier, inc=1, device_id=(r - 1, c, layer), device_id_type=MESH)

    with scope("barrier"):
        pl.semaphore_wait(barrier, 2 * (cols_n + has_next.astype(jnp.int32) + has_prev.astype(jnp.int32)) - 1)

    def part(m, layer):
        return lanes(m * block + layer * half, half)

    def plane_copy(mask, side, s, p, origin, source, device):
        m = member(s, p)
        dst = jr_ref.at[p, m, pl.ds(pl.multiple_of(origin * piece, piece), piece), :]
        return remote(source if source is not None else dst, dst, jr_send.at[mask, side, s, p],
                      jr_recv.at[mask, side, s, p], device)

    def plane_out(s, masks, pairs=range(pair_dev)):
        for mask in masks:
            for p in pairs:
                for side, layer in ((0, l), (1, other)):
                    if mask == 0 and side == 0:
                        continue
                    src = t_ref.at[p, :, part(member(s, p), layer)]
                    send(plane_copy(mask, side, s, p, mine, src, (r, c ^ mask, layer)))

    seen = set()

    def plane_wait(mask, s, p):
        if (mask, s, p) in seen:
            return
        seen.add((mask, s, p))
        for side, layer in ((0, l), (1, other)):
            if mask == 0 and side == 0:
                continue
            plane_copy(mask, side, s, p, (c ^ mask) * 2 + layer, None, partner).wait_recv()

    def plane_relay(s, p, mask):
        plane_wait(mask, s, p)
        for side, layer in ((0, l), (1, other)):
            send(plane_copy(3, side, s, p, (c ^ mask) * 2 + layer, None, (r, c ^ mask ^ 3, l)))

    same = r == c
    differs = r != c
    wide = 2 * piece

    def chip_rows(column):
        return pl.ds(pl.multiple_of(column * wide, wide), wide)

    def left_unit(mask, s, p):
        return jr_ref.at[p, member(s, p), chip_rows(c ^ mask), :]

    def handed(mask, s, p, src):
        return remote(
            src, jo_ref.at[mask, s, p], jo_send.at[mask, s, p], jo_recv.at[mask, s, p], partner
        )

    def halves_out(s):
        for mask in range(cols_n):
            for p in range(pair_dev):
                send(handed(mask, s, p, left_unit(mask, s, p)), same)

    kinds = (0, 1) if square else (0,)

    def carried(kind, s, group, up):
        if not square:
            return True
        side = ((c ^ group) & 1) == 0
        if s == 1:
            return side
        crossed = (group == 1) if up else (group == rows_n - 2)
        return crossed & side if kind else jnp.logical_not(crossed) | side

    def ways():
        return (
            (True, has_next, r + 1, zu_send, zu_recv), (False, has_prev, r - 1, zd_send, zd_recv)
        )

    def rows_out(s):
        for k in range(pair_dev):
            p = leading(r, k)
            for side, layer in ((0, l), (1, other)):
                for up, there, to, _, recv in ways():
                    send(remote(
                        t_ref.at[p, :, part(member(s, p), layer)],
                        z_ref.at[r, 0, s, p, pl.ds(pl.multiple_of(l * piece, piece), piece), :],
                        zo_send.at[int(up), side, s, p], recv.at[1, 0, s, p], (to, c, layer),
                    ), there & carried(0, s, r, up))

    def rows_across(s, among=True):
        for p in range(pair_dev):
            plane_wait(1, s, p)
        for k in range(pair_dev):
            p = leading(r, k)
            for up, there, to, snd, recv in ways():
                send(remote(
                    left_unit(1, s, p), z_ref.at[r, 1, s, p], snd.at[0, 1, s, p], recv.at[1, 1, s, p], (to, c, l)
                ), there & among & carried(1, s, r, up))

    def arrivals(s, step):
        for kind in kinds:
            for up, recv, snd, plane, to, into in (
                (True, zu_recv, zu_send, r - step, r + 1, ju_send),
                (False, zd_recv, zd_send, r + step, r - 1, jd_send),
            ):
                at = jnp.clip(plane, 0, rows_n - 1)
                here = (plane >= 0) & (plane < rows_n) & carried(kind, s, at, up)
                onward = here & (to >= 0) & (to < rows_n)
                yield kind, recv, snd, at, here, onward, to, into

    def hand_over(s, step, among, only=None, ends=None, near=None):
        for k in range(pair_dev):
            for kind, _, _, at, here, onward, _, into in arrivals(s, step):
                p = leading(at, k)
                if only not in (None, kind):
                    continue
                chosen = (onward if among else here & jnp.logical_not(onward)) & (at != c)
                if near is not None:
                    chosen = chosen & ((at == (c ^ 1)) if near else (at != (c ^ 1)))
                if ends is not None:
                    at_end = (at == 0) | (at == rows_n - 1)
                    chosen = chosen & (at_end if ends else jnp.logical_not(at_end))
                mask = (c ^ at) ^ kind
                send(remote(
                    z_ref.at[at, kind, s, p], z_ref.at[at, mask, s, p], into.at[step, kind, s, p],
                    jc_recv.at[mask, s, p], (r, at, l),
                ), chosen)

    def forward(s, step, give=True, only=None, ends=None, clear=None):
        for k in range(pair_dev):
            for kind, recv, snd, at, _, onward, to, _ in arrivals(s, step):
                p = leading(at, k)
                if clear is not None:
                    busy = ((c ^ jnp.where(to > r, 1, rows_n - 2)) & 1) == 0
                    onward = onward & (jnp.logical_not(busy) if clear else busy)
                block_ref = z_ref.at[at, kind, s, p]
                if step + 1 == rows_n or only not in (None, kind):
                    continue
                if ends is not None:
                    at_end = (at == 0) | (at == rows_n - 1)
                    onward = onward & (at_end if ends else jnp.logical_not(at_end))

                @pl.when(onward)
                def _():
                    remote(block_ref, block_ref, snd.at[step, kind, s, p], recv.at[step, kind, s, p],
                           partner).wait_recv()

                send(remote(
                    block_ref, block_ref, snd.at[step, kind, s, p], recv.at[step + 1, kind, s, p], (to, c, l)
                ), onward)
        if give:
            hand_over(s, step, True, only, ends)

    def finish(s, step, near=None):
        for k in range(pair_dev):
            for kind, recv, snd, at, here, onward, _, _ in arrivals(s, step):
                p = leading(at, k)
                block_ref = z_ref.at[at, kind, s, p]

                @pl.when(here & jnp.logical_not(onward))
                def _():
                    remote(block_ref, block_ref, snd.at[step, kind, s, p], recv.at[step, kind, s, p],
                           partner).wait_recv()

        hand_over(s, step, False, near=near)

    def columns_copy(p):
        rows = pl.ds(p * order, order)
        return remote(a_ref.at[rows], ap_ref.at[rows], ap_send.at[p], ap_recv.at[p], partner)

    def split_columns(src, layer, p):
        count = order // ROWS

        def fetch(at):
            slot = lax.rem(at, 2)
            rows = pl.ds(pl.multiple_of(p * order + at * ROWS, ROWS), ROWS)
            for j in range(width):
                for tile in range(tiles):
                    pltpu.make_async_copy(
                        src.at[rows, tile * width + j, 0, :],
                        a_stage.at[slot, :, pl.ds(j * half + tile * LANES, LANES)],
                        stage_sem.at[slot],
                    ).start()

        def body(at, carry):
            @pl.when(at + 1 < count)
            def _():
                fetch(at + 1)

            slot = lax.rem(at, 2)
            pltpu.make_async_copy(a_stage.at[slot], a_stage.at[slot], stage_sem.at[slot]).wait()
            rows = pl.ds(pl.multiple_of(at * ROWS, ROWS), ROWS)
            for j in range(width):
                high, low = halves_of(a_stage[slot, :, j * half : (j + 1) * half])
                cols = lanes(j * block + layer * half, half)
                a_hi[p, rows, cols] = high
                a_lo[p, rows, cols] = low
            return carry

        fetch(0)
        lax.fori_loop(0, count, body, 0)

    def turn(s):
        def fetch(mask):
            for p in range(pair_dev):
                plane_wait(mask, s, p)
            for p in range(pair_dev):
                pltpu.make_async_copy(left_unit(mask, s, p), j_stage.at[mask % 2, p], j_sem.at[mask % 2]).start()

        fetch(0)
        for mask in range(cols_n):
            if mask + 1 < cols_n:
                fetch(mask + 1)
            stage = j_stage.at[mask % 2]
            pltpu.make_async_copy(stage, stage, j_sem.at[mask % 2]).wait()
            at = lanes((c ^ mask) * wide, wide)
            for p in range(pair_dev):
                high, low = halves_of(j_stage[mask % 2, p].T)
                jt_hi[slot_of(s, p), :, at] = high
                jt_lo[slot_of(s, p), :, at] = low
        halves_out(s)

    def left(slot):
        p = slot // 2
        kept = slot in (0, width - 1)
        at = (jnp.where(has_prev, 2, 0) if slot == 0 else 1) if kept else None

        def body(n, carry):
            cols = lanes(n * block, block)
            x = three_dots(jt_hi[slot], jt_lo[slot], a_hi[p, :, cols], a_lo[p, :, cols])
            if kept:
                high, low = halves_of(x)
                lr_hi[at, :, cols] = high
                lr_lo[at, :, cols] = low
            else:
                l_tile[(slot - 1) * width + n] = x
            return carry

        lax.fori_loop(0, width, body, 0)

    def left_out(slot, order_of_tiles):
        if slot == 1:
            moved, target, at = has_prev, r - 1, jnp.where(has_prev, 3, 2)
        else:
            moved, target, at = has_next, r + 1, jnp.where(has_next, 0, 3)
        for n in order_of_tiles:
            src, dst = l_tile.at[(slot - 1) * width + n], lr_ref.at[at, n]
            send(remote(src, dst, lr_send.at[slot, n], lr_recv.at[at, n], (target, c, l)), moved)
            pl.when(jnp.logical_not(moved))(pltpu.make_async_copy(src, dst, lr_recv.at[at, n]).start)

    def right_pieces(s, p):
        depth = j_stage.shape[0] * pair_dev
        for mask in range(cols_n):
            unit = z_ref.at[c, mask, s, p]
            late = differs
            if square and mask == 1:
                late = differs & jnp.logical_not(jnp.where(r > c, c == 1, c == rows_n - 2))
            if mask and not (square and mask == 1 and s == 1):
                @pl.when(late)
                def _():
                    remote(unit, unit, jo_send.at[mask, s, p], jc_recv.at[mask, s, p], partner).wait_recv()

            send(handed(mask, s, p, unit), differs)
        jobs = [(side, mask) for side in range(2) for mask in range(cols_n)]

        def place(k):
            at = k % depth
            return j_stage.at[at // pair_dev, at % pair_dev], j_sem.at[at]

        def fetch(k):
            side, mask = jobs[k]

            def take(src):
                return pltpu.make_async_copy(src, *place(k))

            if side:
                src = jo_ref.at[mask, s, p]
                handed(mask, s, p, src).wait_recv()
                take(src).start()
            else:
                pl.when(differs)(take(z_ref.at[c, mask, s, p]).start)
                pl.when(same)(take(left_unit(mask, s, p)).start)

        ahead = depth - 1
        for k in range(min(ahead, len(jobs))):
            fetch(k)
        for k, (side, mask) in enumerate(jobs):
            if k + ahead < len(jobs):
                fetch(k + ahead)
            stage, sem = place(k)
            pltpu.make_async_copy(stage, stage, sem).wait()
            cols = lanes((other if side else l) * half, half)
            high, low = halves_of(stage[...])
            jc_hi[slot_of(s, p), chip_rows(c ^ mask), cols] = high
            jc_lo[slot_of(s, p), chip_rows(c ^ mask), cols] = low

    def left_rows(at, q):
        loads = []
        for n in range(2):
            src = lr_ref.at[at, 2 * q + n]
            pltpu.make_async_copy(src, src, lr_recv.at[at, 2 * q + n]).wait()
            loads.append(pltpu.make_async_copy(src, l_stage.at[n], stage_sem.at[n]))
            loads[-1].start()
        for n in range(2):
            loads[n].wait()
            high, low = halves_of(l_stage[n])
            cols = lanes((2 * q + n) * block, block)
            lr_hi[at, :, cols] = high
            lr_lo[at, :, cols] = low

    left_end, right_end = c > 0, c + 1 < cols_n
    staying, arriving = (1, width - 2), (0, width - 1)
    by_way = staying if square else ()
    low_rows = pl.ds(pl.multiple_of(l * half, half), half)

    def right_tile(at, j, q):
        rows = lanes(q * order, order)
        tile = at * width + j
        o_tile[tile] = three_dots(lr_hi[at, :, rows], lr_lo[at, :, rows], jc_hi[j], jc_lo[j])
        return tile

    def right_moving(at, q):
        j = 1 + q
        tile = right_tile(at, j, q)
        up = q == 1
        moved = jnp.where(up, right_end, left_end)
        target = jnp.where(up, c + 1, c - 1)
        slot = jnp.where(up, jnp.where(right_end, 0, 3), jnp.where(left_end, 3, 2))
        column = jnp.where(moved, target, c)
        dst = out_ref.at[slot, at, low_rows, :]
        around = None
        if isinstance(at, int) and at in by_way:
            around = jnp.where(up, c == 1, c == 2)
        for s, layer in ((0, l), (1, other)):
            src = o_tile.at[tile, :, lanes(layer * half, half)]
            condition = moved if s == 0 else None
            if around is not None:
                index = by_way.index(at)
                send(remote(
                    src, via_ref.at[index, l], o_send.at[tile, s], via_recv.at[index, l], (r, c ^ 2, layer)
                ), around)
                direct = jnp.logical_not(around)
                condition = direct if condition is None else condition & direct
            send(remote(src, dst, o_send.at[tile, s], o_recv.at[slot, l], (r, column, layer)), condition)
            if s == 0:
                pl.when(jnp.logical_not(moved))(pltpu.make_async_copy(src, dst, o_recv.at[slot, l]).start)

    def right_kept(at, j):
        tile = right_tile(at, j, j // 2)
        slot = jnp.where(left_end, 2, 0) if j == 0 else 1
        dst = out_ref.at[slot, at, low_rows, :]
        send(remote(
            o_tile.at[tile, :, lanes(other * half, half)], dst, o_send.at[tile, 1], o_recv.at[slot, l], partner
        ))
        pltpu.make_async_copy(
            o_tile.at[tile, :, lanes(l * half, half)], dst, o_recv.at[slot, l]
        ).start()

    def right_relay(index):
        outer = (c == 0) | (c == cols_n - 1)
        slot = jnp.where(c == 0, 3, 0)
        for layer in range(2):
            src = via_ref.at[index, layer]
            rows = pl.ds(layer * half, half)

            @pl.when(outer)
            def _():
                remote(src, src, via_send.at[index, layer], via_recv.at[index, layer], partner).wait_recv()

            send(remote(
                src, out_ref.at[slot, by_way[index], rows, :], via_send.at[index, layer], o_recv.at[slot, layer],
                (r, c ^ 1, l),
            ), outer)

    rows_out(0)
    if square:
        plane_out(0, (1, 2, 0))
        plane_out(1, (1, 0))
    else:
        for s in range(2):
            plane_out(s, list(range(1, cols_n)) + [0])
    for p in range(pair_dev):
        send(columns_copy(p))
    load = pltpu.make_async_copy(t_ref, own_v, own_sem.at[0, 0, 0])
    load.start()
    load.wait()
    fills = []
    for s in range(2):
        for p in range(pair_dev):
            fills.append(pltpu.make_async_copy(
                own_v.at[p, :, part(member(s, p), l)],
                jr_ref.at[p, member(s, p), pl.ds(pl.multiple_of(mine * piece, piece), piece), :],
                own_sem.at[1, s, p],
            ))
    for copy in fills:
        copy.start()
    with scope("split_own"):
        for p in range(pair_dev):
            split_columns(a_ref, l, p)
    for copy in fills:
        copy.wait()
    if square:
        with scope("relay0"):
            for p in range(pair_dev):
                plane_relay(0, p, 1)
        plane_out(1, (2,))
        rows_across(0)
    with scope("fwd_a1"):
        forward(0, 1, only=0)
    rows_out(1)
    with scope("split_p0"):
        columns_copy(0).wait_recv()
        split_columns(ap_ref, other, 0)
    with scope("split_p1"):
        for p in range(1, pair_dev):
            columns_copy(p).wait_recv()
            split_columns(ap_ref, other, p)
    if square:
        with scope("fwd_a1x"):
            forward(0, 1, only=1)
        at_end = jnp.logical_not(has_prev & has_next)
        with scope("across1"):
            rows_across(1, at_end)
    with scope("fin_a1"):
        finish(0, 1, near=True)
    with scope("fwd_b1e0"):
        forward(1, 1, only=0, ends=True)
    if square:
        for step in range(2, rows_n - 1):
            with scope("fwd_a2c"):
                forward(0, step, False, clear=True)
    with scope("turn_a"):
        turn(0)
    with scope("left_a2"):
        left(width - 2)
    for step in range(2, rows_n - 1):
        with scope("fwd_a2"):
            forward(0, step, False, clear=False if square else None)
    if square:
        rows_across(1, jnp.logical_not(at_end))
        with scope("fwd_b1e"):
            forward(1, 1, only=1, ends=True)
    with scope("left_a1"):
        left(1)
    if square:
        with scope("relay1"):
            for p in range(pair_dev):
                plane_relay(1, p, 2)
    for step in range(2, rows_n - 1):
        hand_over(0, step, True)
    hand_over(0, 1, False, near=False)
    for step in range(2, rows_n):
        with scope("fin_a"):
            finish(0, step)
    for step in range(2, rows_n - 1):
        with scope("fwd_b2"):
            forward(1, step)
    with scope("fwd_b1m0"):
        forward(1, 1, only=0, ends=False)
    with scope("turn_b"):
        turn(1)
    with scope("left_b"):
        for slot in (width - 1, 0):
            left(slot)
    if square:
        with scope("fwd_b1m"):
            forward(1, 1, only=1, ends=False)
    first, last = (0, 1), (2, 3)
    for tiles_first, tiles_last in ((first, last), (last, first)):
        left_out(width - 2, tiles_first)
        left_out(1, tiles_last)
    with scope("rows"):
        @pl.when(jnp.logical_not(has_prev))
        def _():
            for q in range(pair_dev):
                left_rows(2, q)
    for k in range(pair_dev):
        q = leading(c, k)
        with scope("pieces_a"):
            right_pieces(0, q)
        with scope("right"):
            for at in staying:
                right_moving(at, q)

    first, last = jnp.logical_not(has_prev), jnp.logical_not(has_next)

    def arrived(at, q):
        with scope("rows_arr"):
            @pl.when(has_prev | (at == width - 1))
            def _():
                left_rows(at, q)
        with scope("right"):
            right_moving(at, q)

    top, low = 0, width - 1
    arrived(jnp.where(last, low, top), jnp.where(last, 1, 0))
    arrived(jnp.where(first, top, low), jnp.where(last, 0, 1))
    for step in range(1, rows_n):
        with scope("fin_b"):
            finish(1, step)
    if square:
        with scope("via0"):
            right_relay(0)
            right_relay(1)
    arrived(jnp.where(first, low, top), jnp.where(last, 0, 1))
    arrived(jnp.where(last, top, low), jnp.where(last, 1, 0))
    with scope("pieces_b"):
        for p in range(pair_dev):
            right_pieces(1, p)
    with scope("right_local"):
        for at in staying + arriving:
            for j in (0, width - 1):
                right_kept(at, j)

    with scope("out_wait"):
        for slot in range(width):
            for layer in range(2):
                block_ref = out_ref.at[slot, :, pl.ds(layer * half, half), :]
                pltpu.make_async_copy(block_ref, block_ref, o_recv.at[slot, layer]).wait()
    with scope("send_wait"):
        for copy, condition in pending:
            if condition is None:
                copy.wait_send()
            else:
                pl.when(condition)(copy.wait_send)


def spread(size, x_ref, o_ref, buffer, in_sem, out_sem):
    width, block, tiles = size
    rows = buffer.shape[2]
    steps = block // rows

    def inward(k):
        i, at = k // steps, k % steps
        return pltpu.make_async_copy(x_ref.at[:, i, pl.ds(at * rows, rows), :], buffer.at[k], in_sem.at[k])

    def outward(k, j, tile):
        return pltpu.make_async_copy(
            buffer.at[k, j, :, pl.ds(tile * LANES, LANES)],
            o_ref.at[pl.ds(k * rows, rows), tile * width + j, 0, :], out_sem.at[k, j, tile],
        )

    every = range(width * steps)
    for k in every:
        inward(k).start()
    for k in every:
        inward(k).wait()
        for j in range(width):
            for tile in range(tiles):
                outward(k, j, tile).start()
    for k in every:
        for j in range(width):
            for tile in range(tiles):
                outward(k, j, tile).wait()


def shards(matrix, transforms):
    width, block, _, half = matrix.shape
    pair_dev = width // 2
    order = 2 * block
    rows_n, cols_n = lax.axis_size("row"), lax.axis_size("col")
    tiles = half // LANES
    raw_shape = (width * block, width * tiles, 1, LANES)
    own = transforms[0]
    piece = own.shape[1]
    f32, bf16 = jnp.float32, jnp.bfloat16

    raw = matrix.reshape(width * block, width, tiles, LANES).transpose(0, 2, 1, 3).reshape(raw_shape)
    any_space = pl.BlockSpec(memory_space=pl.ANY)
    dma = pltpu.SemaphoreType.DMA
    vmem = pltpu.VMEM
    by_piece = (2, pair_dev)
    by_unit = by_piece + (2 * piece, half)
    flops = 3 * 2 * 2 * width * half * order * width * block
    outs = pl.pallas_call(
        functools.partial(sweep, (rows_n, cols_n, pair_dev, width, block, half, piece)),
        name="sweep",
        out_shape=[
            jax.ShapeDtypeStruct((width, width, block, half), f32),
            jax.ShapeDtypeStruct(raw_shape, f32),
            jax.ShapeDtypeStruct((pair_dev, 2, order, half), f32),
            jax.ShapeDtypeStruct((cols_n,) + by_unit, f32),
            jax.ShapeDtypeStruct((rows_n, cols_n) + by_unit, f32),
            jax.ShapeDtypeStruct((width, width, half, block), f32),
            jax.ShapeDtypeStruct((2, 2, half, half), f32),
        ],
        in_specs=[any_space, any_space],
        out_specs=[any_space] * 7,
        scratch_shapes=[
            vmem((pair_dev, order, width * block), bf16),
            vmem((pair_dev, order, width * block), bf16),
            vmem((width, half, order), bf16),
            vmem((width, half, order), bf16),
            vmem((width, order, block), bf16),
            vmem((width, order, block), bf16),
            vmem((width, half, width * block), bf16),
            vmem((width, half, width * block), bf16),
            vmem((2 * width, half, block), f32),
            vmem((width * width, half, block), f32),
            vmem((pair_dev, piece, order), f32),
            vmem((2, ROWS, width * half), f32),
            vmem((4, pair_dev, 2 * piece, half), f32),
            vmem((2, half, block), f32),
            dma((2,)), dma((4 * pair_dev,)), dma((2,) + by_piece),
            dma((pair_dev,)), dma((pair_dev,)),
            dma((cols_n, 2) + by_piece), dma((cols_n, 2) + by_piece),
            dma((2, 2) + by_piece),
            dma((rows_n, 2) + by_piece), dma((rows_n, 2) + by_piece),
            dma((rows_n, 2) + by_piece), dma((rows_n, 2) + by_piece),
            dma((rows_n, 2) + by_piece), dma((rows_n, 2) + by_piece), dma((cols_n,) + by_piece),
            dma((cols_n,) + by_piece), dma((cols_n,) + by_piece),
            dma((width, width)), dma((width, width)),
            dma((width * width, 2)), dma((width, 2)),
            dma((2, 2)), dma((2, 2)),
        ],
        compiler_params=pltpu.CompilerParams(
            collective_id=0, has_side_effects=True, vmem_limit_bytes=VMEM_LIMIT
        ),
        cost_estimate=pl.CostEstimate(flops=flops, bytes_accessed=0, transcendentals=0),
    )(raw, own)
    blocks = outs[0]

    steps = width * block // ROWS
    result = pl.pallas_call(
        functools.partial(spread, (width, block, tiles)),
        name="spread",
        in_specs=[any_space],
        out_specs=any_space,
        out_shape=jax.ShapeDtypeStruct(raw_shape, f32),
        scratch_shapes=[
            vmem((steps, width, ROWS, half), f32), dma((steps,)), dma((steps, width, tiles)),
        ],
    )(blocks)
    result = result.reshape(width, block, tiles, width, LANES).transpose(0, 1, 3, 2, 4)
    return result.reshape(width, block, width, half)


def solution(mesh):
    return jax.shard_map(
        shards,
        mesh=mesh,
        in_specs=(P("row", None, "col", "layer"), P(None, "row", ("col", "layer"), None)),
        out_specs=P("row", None, "col", "layer"),
        check_vma=False,
    )
```

```python
import functools

import jax
import jax.numpy as jnp
from jax import lax
from jax.experimental import pallas as pl
from jax.experimental.pallas import tpu as pltpu
from jax.sharding import PartitionSpec as P

MESH = pl.DeviceIdType.MESH
LANES = 128
ROWS = 256
VMEM_LIMIT = 66_000_000
scope = jax.named_scope


def halves_of(x):
    high = x.astype(jnp.bfloat16)
    low = (x - high.astype(jnp.float32)).astype(jnp.bfloat16)
    return high, low


def three_dots(a_high, a_low, b_high, b_low):
    def dot(a, b):
        return lax.dot_general(a, b, (((1,), (0,)), ((), ())), preferred_element_type=jnp.float32)

    return dot(a_high, b_high) + (dot(a_high, b_low) + dot(a_low, b_high))


def sweep(
    size,
    a_ref, t_ref,
    out_ref, ap_ref, jr_ref, jo_ref, z_ref, lr_ref, via_ref,
    a_hi, a_lo, jt_hi, jt_lo, jc_hi, jc_lo, lr_hi, lr_lo, l_tile, o_tile,
    own_v, a_stage, j_stage, l_stage,
    stage_sem, j_sem, own_sem,
    ap_send, ap_recv, jr_send, jr_recv,
    zo_send, zu_send, zu_recv, zd_send, zd_recv,
    ju_send, jd_send, jc_recv, jo_send, jo_recv,
    lr_send, lr_recv, o_send, o_recv, via_send, via_recv,
):
    rows_n, cols_n, pair_dev, width, block, half, piece = size
    order = 2 * block
    tiles = half // LANES
    r = lax.axis_index("row")
    c = lax.axis_index("col")
    l = lax.axis_index("layer")
    other = 1 - l
    partner = (r, c, other)
    mine = c * 2 + l
    square = cols_n == 4
    pending = []

    def remote(src, dst, send, recv, device):
        return pltpu.make_async_remote_copy(
            src_ref=src, dst_ref=dst, send_sem=send, recv_sem=recv, device_id=device, device_id_type=MESH
        )

    def go(copy, condition=None):
        if condition is None:
            copy.start()
        else:
            pl.when(condition)(copy.start)

    def drain(sem, ref, condition=None):
        pending.append((pltpu.make_async_copy(ref, ref, sem).wait, condition))

    def send(copy, condition=None):
        go(copy, condition)
        pending.append((copy.wait_send, condition))

    def lanes(start, count):
        return pl.ds(pl.multiple_of(start, LANES), count)

    def member(s, p):
        return 1 - p if s == 0 else p

    def leading(group, k):
        return jnp.where((group & 1) == 0 if square else group == 0, 1 - k, k)

    def slot_of(s, p):
        return 2 * p + member(s, p)

    barrier = pltpu.get_barrier_semaphore()
    for mask in range(cols_n):
        for layer in (l, other):
            if mask == 0 and layer is l:
                continue
            pl.semaphore_signal(barrier, inc=1, device_id=(r, c ^ mask, layer), device_id_type=MESH)
    has_next = r + 1 < rows_n
    has_prev = r > 0

    for layer in (l, other):
        @pl.when(has_next)
        def _():
            pl.semaphore_signal(barrier, inc=1, device_id=(r + 1, c, layer), device_id_type=MESH)

        @pl.when(has_prev)
        def _():
            pl.semaphore_signal(barrier, inc=1, device_id=(r - 1, c, layer), device_id_type=MESH)

    with scope("barrier"):
        pl.semaphore_wait(barrier, 2 * (cols_n + has_next.astype(jnp.int32) + has_prev.astype(jnp.int32)) - 1)

    def part(m, layer):
        return lanes(m * block + layer * half, half)

    def plane_copy(mask, side, s, p, origin, source, device):
        m = member(s, p)
        dst = jr_ref.at[p, m, pl.ds(pl.multiple_of(origin * piece, piece), piece), :]
        return remote(source if source is not None else dst, dst, jr_send.at[0],
                      jr_recv.at[mask, side, s, p], device)

    def plane_out(s, masks, pairs=range(pair_dev)):
        for mask in masks:
            for p in pairs:
                for side, layer in ((0, l), (1, other)):
                    if mask == 0 and side == 0:
                        continue
                    src = t_ref.at[p, :, part(member(s, p), layer)]
                    go(plane_copy(mask, side, s, p, mine, src, (r, c ^ mask, layer)))

    seen = set()

    def plane_wait(mask, s, p):
        if (mask, s, p) in seen:
            return
        seen.add((mask, s, p))
        for side, layer in ((0, l), (1, other)):
            if mask == 0 and side == 0:
                continue
            plane_copy(mask, side, s, p, (c ^ mask) * 2 + layer, None, partner).wait_recv()

    def plane_relay(s, p, mask):
        plane_wait(mask, s, p)
        for side, layer in ((0, l), (1, other)):
            go(plane_copy(3, side, s, p, (c ^ mask) * 2 + layer, None, (r, c ^ mask ^ 3, l)))

    same = r == c
    differs = r != c
    wide = 2 * piece

    def chip_rows(column):
        return pl.ds(pl.multiple_of(column * wide, wide), wide)

    def left_unit(mask, s, p):
        return jr_ref.at[p, member(s, p), chip_rows(c ^ mask), :]

    def handed(mask, s, p, src):
        return remote(
            src, jo_ref.at[mask, s, p], jo_send.at[0], jo_recv.at[mask, s, p], partner
        )

    def halves_out(s):
        for mask in range(cols_n):
            for p in range(pair_dev):
                go(handed(mask, s, p, left_unit(mask, s, p)), same)

    kinds = (0, 1) if square else (0,)

    def carried(kind, s, group, up):
        if not square:
            return True
        side = ((c ^ group) & 1) == 0
        if s == 1:
            return side
        crossed = (group == 1) if up else (group == rows_n - 2)
        return crossed & side if kind else jnp.logical_not(crossed) | side

    def ways():
        return (
            (True, has_next, r + 1, zu_send, zu_recv), (False, has_prev, r - 1, zd_send, zd_recv)
        )

    def rows_out(s):
        for k in range(pair_dev):
            p = leading(r, k)
            for side, layer in ((0, l), (1, other)):
                for up, there, to, _, recv in ways():
                    go(remote(
                        t_ref.at[p, :, part(member(s, p), layer)],
                        z_ref.at[r, 0, s, p, pl.ds(pl.multiple_of(l * piece, piece), piece), :],
                        zo_send.at[int(up), s], recv.at[1, 0, s, p], (to, c, layer),
                    ), there & carried(0, s, r, up))
        for up, there, _, _, _ in ways():
            drain(zo_send.at[int(up), s], z_ref.at[0, 0, s], there & carried(0, s, r, up))

    def rows_across(s, among=True):
        for p in range(pair_dev):
            plane_wait(1, s, p)
        for k in range(pair_dev):
            p = leading(r, k)
            for up, there, to, snd, recv in ways():
                go(remote(
                    left_unit(1, s, p), z_ref.at[r, 1, s, p], snd.at[0, 1, s], recv.at[1, 1, s, p], (to, c, l)
                ), there & among & carried(1, s, r, up))
        for up, there, _, snd, _ in ways():
            drain(snd.at[0, 1, s], z_ref.at[0, 0, s], there & among & carried(1, s, r, up))

    def arrivals(s, step):
        for kind in kinds:
            for up, recv, snd, plane, to, into in (
                (True, zu_recv, zu_send, r - step, r + 1, ju_send),
                (False, zd_recv, zd_send, r + step, r - 1, jd_send),
            ):
                at = jnp.clip(plane, 0, rows_n - 1)
                here = (plane >= 0) & (plane < rows_n) & carried(kind, s, at, up)
                onward = here & (to >= 0) & (to < rows_n)
                yield kind, recv, snd, at, here, onward, to, into

    def hand_over(s, step, among, only=None, ends=None, near=None):
        for k in range(pair_dev):
            for kind, _, _, at, here, onward, _, into in arrivals(s, step):
                p = leading(at, k)
                if only not in (None, kind):
                    continue
                chosen = (onward if among else here & jnp.logical_not(onward)) & (at != c)
                if near is not None:
                    chosen = chosen & ((at == (c ^ 1)) if near else (at != (c ^ 1)))
                if ends is not None:
                    at_end = (at == 0) | (at == rows_n - 1)
                    chosen = chosen & (at_end if ends else jnp.logical_not(at_end))
                mask = (c ^ at) ^ kind
                go(remote(
                    z_ref.at[at, kind, s, p], z_ref.at[at, mask, s, p], into.at[step, kind, s],
                    jc_recv.at[mask, s, p], (r, at, l),
                ), chosen)
                if k + 1 == pair_dev:
                    drain(into.at[step, kind, s], z_ref.at[0, 0, s], chosen)

    def forward(s, step, give=True, only=None, ends=None, clear=None):
        for k in range(pair_dev):
            for kind, recv, snd, at, _, onward, to, _ in arrivals(s, step):
                p = leading(at, k)
                if clear is not None:
                    busy = ((c ^ jnp.where(to > r, 1, rows_n - 2)) & 1) == 0
                    onward = onward & (jnp.logical_not(busy) if clear else busy)
                block_ref = z_ref.at[at, kind, s, p]
                if step + 1 == rows_n or only not in (None, kind):
                    continue
                if ends is not None:
                    at_end = (at == 0) | (at == rows_n - 1)
                    onward = onward & (at_end if ends else jnp.logical_not(at_end))

                @pl.when(onward)
                def _():
                    remote(block_ref, block_ref, snd.at[step, kind, s], recv.at[step, kind, s, p],
                           partner).wait_recv()

                go(remote(
                    block_ref, block_ref, snd.at[step, kind, s], recv.at[step + 1, kind, s, p], (to, c, l)
                ), onward)
                if k + 1 == pair_dev:
                    drain(snd.at[step, kind, s], z_ref.at[0, 0, s], onward)
        if give:
            hand_over(s, step, True, only, ends)

    def finish(s, step, near=None):
        for k in range(pair_dev):
            for kind, recv, snd, at, here, onward, _, _ in arrivals(s, step):
                p = leading(at, k)
                block_ref = z_ref.at[at, kind, s, p]

                @pl.when(here & jnp.logical_not(onward))
                def _():
                    remote(block_ref, block_ref, snd.at[step, kind, s], recv.at[step, kind, s, p],
                           partner).wait_recv()

        hand_over(s, step, False, near=near)

    def columns_copy(p):
        rows = pl.ds(p * order, order)
        return remote(a_ref.at[rows], ap_ref.at[rows], ap_send.at[p], ap_recv.at[p], partner)

    def split_columns(src, layer, p):
        count = order // ROWS

        def fetch(at):
            slot = lax.rem(at, 2)
            rows = pl.ds(pl.multiple_of(p * order + at * ROWS, ROWS), ROWS)
            for j in range(width):
                for tile in range(tiles):
                    pltpu.make_async_copy(
                        src.at[rows, tile * width + j, 0, :],
                        a_stage.at[slot, :, pl.ds(j * half + tile * LANES, LANES)],
                        stage_sem.at[slot],
                    ).start()

        def body(at, carry):
            @pl.when(at + 1 < count)
            def _():
                fetch(at + 1)

            slot = lax.rem(at, 2)
            pltpu.make_async_copy(a_stage.at[slot], a_stage.at[slot], stage_sem.at[slot]).wait()
            rows = pl.ds(pl.multiple_of(at * ROWS, ROWS), ROWS)
            for j in range(width):
                high, low = halves_of(a_stage[slot, :, j * half : (j + 1) * half])
                cols = lanes(j * block + layer * half, half)
                a_hi[p, rows, cols] = high
                a_lo[p, rows, cols] = low
            return carry

        fetch(0)
        lax.fori_loop(0, count, body, 0)

    def turn(s):
        def fetch(mask):
            for p in range(pair_dev):
                plane_wait(mask, s, p)
            for p in range(pair_dev):
                pltpu.make_async_copy(left_unit(mask, s, p), j_stage.at[mask % 2, p], j_sem.at[mask % 2]).start()

        fetch(0)
        for mask in range(cols_n):
            if mask + 1 < cols_n:
                fetch(mask + 1)
            stage = j_stage.at[mask % 2]
            pltpu.make_async_copy(stage, stage, j_sem.at[mask % 2]).wait()
            at = lanes((c ^ mask) * wide, wide)
            for p in range(pair_dev):
                high, low = halves_of(j_stage[mask % 2, p].T)
                jt_hi[slot_of(s, p), :, at] = high
                jt_lo[slot_of(s, p), :, at] = low
        halves_out(s)

    def left(slot):
        p = slot // 2
        kept = slot in (0, width - 1)
        at = (jnp.where(has_prev, 2, 0) if slot == 0 else 1) if kept else None

        def body(n, carry):
            cols = lanes(n * block, block)
            x = three_dots(jt_hi[slot], jt_lo[slot], a_hi[p, :, cols], a_lo[p, :, cols])
            if kept:
                high, low = halves_of(x)
                lr_hi[at, :, cols] = high
                lr_lo[at, :, cols] = low
            else:
                l_tile[(slot - 1) * width + n] = x
            return carry

        lax.fori_loop(0, width, body, 0)

    def left_out(slot, order_of_tiles):
        if slot == 1:
            moved, target, at = has_prev, r - 1, jnp.where(has_prev, 3, 2)
        else:
            moved, target, at = has_next, r + 1, jnp.where(has_next, 0, 3)
        for n in order_of_tiles:
            src, dst = l_tile.at[(slot - 1) * width + n], lr_ref.at[at, n]
            go(remote(src, dst, lr_send.at[slot - 1], lr_recv.at[at, n], (target, c, l)), moved)
            pl.when(jnp.logical_not(moved))(pltpu.make_async_copy(src, dst, lr_recv.at[at, n]).start)

    def right_pieces(s, p):
        depth = j_stage.shape[0] * pair_dev
        for mask in range(cols_n):
            unit = z_ref.at[c, mask, s, p]
            late = differs
            if square and mask == 1:
                late = differs & jnp.logical_not(jnp.where(r > c, c == 1, c == rows_n - 2))
            if mask and not (square and mask == 1 and s == 1):
                @pl.when(late)
                def _():
                    remote(unit, unit, jo_send.at[0], jc_recv.at[mask, s, p], partner).wait_recv()

            go(handed(mask, s, p, unit), differs)
        jobs = [(side, mask) for side in range(2) for mask in range(cols_n)]

        def place(k):
            at = k % depth
            return j_stage.at[at // pair_dev, at % pair_dev], j_sem.at[at]

        def fetch(k):
            side, mask = jobs[k]

            def take(src):
                return pltpu.make_async_copy(src, *place(k))

            if side:
                src = jo_ref.at[mask, s, p]
                handed(mask, s, p, src).wait_recv()
                take(src).start()
            else:
                pl.when(differs)(take(z_ref.at[c, mask, s, p]).start)
                pl.when(same)(take(left_unit(mask, s, p)).start)

        ahead = depth - 1
        for k in range(min(ahead, len(jobs))):
            fetch(k)
        for k, (side, mask) in enumerate(jobs):
            if k + ahead < len(jobs):
                fetch(k + ahead)
            stage, sem = place(k)
            pltpu.make_async_copy(stage, stage, sem).wait()
            cols = lanes((other if side else l) * half, half)
            high, low = halves_of(stage[...])
            jc_hi[slot_of(s, p), chip_rows(c ^ mask), cols] = high
            jc_lo[slot_of(s, p), chip_rows(c ^ mask), cols] = low

    def left_rows(at, q):
        loads = []
        for n in range(2):
            src = lr_ref.at[at, 2 * q + n]
            pltpu.make_async_copy(src, src, lr_recv.at[at, 2 * q + n]).wait()
            loads.append(pltpu.make_async_copy(src, l_stage.at[n], stage_sem.at[n]))
            loads[-1].start()
        for n in range(2):
            loads[n].wait()
            high, low = halves_of(l_stage[n])
            cols = lanes((2 * q + n) * block, block)
            lr_hi[at, :, cols] = high
            lr_lo[at, :, cols] = low

    left_end, right_end = c > 0, c + 1 < cols_n
    staying, arriving = (1, width - 2), (0, width - 1)
    by_way = staying if square else ()
    low_rows = pl.ds(pl.multiple_of(l * half, half), half)

    def right_tile(at, j, q):
        rows = lanes(q * order, order)
        tile = at * width + j
        o_tile[tile] = three_dots(lr_hi[at, :, rows], lr_lo[at, :, rows], jc_hi[j], jc_lo[j])
        return tile

    def right_moving(at, q):
        j = 1 + q
        tile = right_tile(at, j, q)
        up = q == 1
        moved = jnp.where(up, right_end, left_end)
        target = jnp.where(up, c + 1, c - 1)
        slot = jnp.where(up, jnp.where(right_end, 0, 3), jnp.where(left_end, 3, 2))
        column = jnp.where(moved, target, c)
        dst = out_ref.at[slot, at, low_rows, :]
        around = None
        if isinstance(at, int) and at in by_way:
            around = jnp.where(up, c == 1, c == 2)
        for s, layer in ((0, l), (1, other)):
            src = o_tile.at[tile, :, lanes(layer * half, half)]
            condition = moved if s == 0 else None
            if around is not None:
                index = by_way.index(at)
                go(remote(
                    src, via_ref.at[index, l], o_send.at[0 if s else 1 + q], via_recv.at[index, l], (r, c ^ 2, layer)
                ), around)
                direct = jnp.logical_not(around)
                condition = direct if condition is None else condition & direct
            go(remote(src, dst, o_send.at[0 if s else 1 + q], o_recv.at[slot, l], (r, column, layer)), condition)
            if s == 0:
                pl.when(jnp.logical_not(moved))(pltpu.make_async_copy(src, dst, o_recv.at[slot, l]).start)

    def right_kept(at, j):
        tile = right_tile(at, j, j // 2)
        slot = jnp.where(left_end, 2, 0) if j == 0 else 1
        dst = out_ref.at[slot, at, low_rows, :]
        go(remote(
            o_tile.at[tile, :, lanes(other * half, half)], dst, o_send.at[0], o_recv.at[slot, l], partner
        ))
        pltpu.make_async_copy(
            o_tile.at[tile, :, lanes(l * half, half)], dst, o_recv.at[slot, l]
        ).start()

    def right_relay(index):
        outer = (c == 0) | (c == cols_n - 1)
        slot = jnp.where(c == 0, 3, 0)
        for layer in range(2):
            src = via_ref.at[index, layer]
            rows = pl.ds(layer * half, half)

            @pl.when(outer)
            def _():
                remote(src, src, via_send.at[index, layer], via_recv.at[index, layer], partner).wait_recv()

            send(remote(
                src, out_ref.at[slot, by_way[index], rows, :], via_send.at[index, layer], o_recv.at[slot, layer],
                (r, c ^ 1, l),
            ), outer)

    rows_out(0)
    if square:
        plane_out(0, (1, 2, 0))
        plane_out(1, (1, 0))
    else:
        for s in range(2):
            plane_out(s, list(range(1, cols_n)) + [0])
    for p in range(pair_dev):
        send(columns_copy(p))
    load = pltpu.make_async_copy(t_ref, own_v, own_sem.at[0, 0, 0])
    load.start()
    load.wait()
    fills = []
    for s in range(2):
        for p in range(pair_dev):
            fills.append(pltpu.make_async_copy(
                own_v.at[p, :, part(member(s, p), l)],
                jr_ref.at[p, member(s, p), pl.ds(pl.multiple_of(mine * piece, piece), piece), :],
                own_sem.at[1, s, p],
            ))
    for copy in fills:
        copy.start()
    with scope("split_own"):
        for p in range(pair_dev):
            split_columns(a_ref, l, p)
    for copy in fills:
        copy.wait()
    if square:
        with scope("relay0"):
            for p in range(pair_dev):
                plane_relay(0, p, 1)
        plane_out(1, (2,))
        rows_across(0)
    with scope("fwd_a1"):
        forward(0, 1, only=0)
    rows_out(1)
    with scope("split_p0"):
        columns_copy(0).wait_recv()
        split_columns(ap_ref, other, 0)
    with scope("split_p1"):
        for p in range(1, pair_dev):
            columns_copy(p).wait_recv()
            split_columns(ap_ref, other, p)
    if square:
        with scope("fwd_a1x"):
            forward(0, 1, only=1)
        at_end = jnp.logical_not(has_prev & has_next)
        with scope("across1"):
            rows_across(1, at_end)
    with scope("fin_a1"):
        finish(0, 1, near=True)
    with scope("fwd_b1e0"):
        forward(1, 1, only=0, ends=True)
    if square:
        for step in range(2, rows_n - 1):
            with scope("fwd_a2c"):
                forward(0, step, False, clear=True)
    with scope("turn_a"):
        turn(0)
    with scope("left_a2"):
        left(width - 2)
    for step in range(2, rows_n - 1):
        with scope("fwd_a2"):
            forward(0, step, False, clear=False if square else None)
    if square:
        rows_across(1, jnp.logical_not(at_end))
        with scope("fwd_b1e"):
            forward(1, 1, only=1, ends=True)
    with scope("left_a1"):
        left(1)
    if square:
        with scope("relay1"):
            for p in range(pair_dev):
                plane_relay(1, p, 2)
    for step in range(2, rows_n - 1):
        hand_over(0, step, True)
    hand_over(0, 1, False, near=False)
    for step in range(2, rows_n):
        with scope("fin_a"):
            finish(0, step)
    for step in range(2, rows_n - 1):
        with scope("fwd_b2"):
            forward(1, step)
    with scope("fwd_b1m0"):
        forward(1, 1, only=0, ends=False)
    with scope("turn_b"):
        turn(1)
    with scope("left_b"):
        left(width - 1)
    if square:
        with scope("fwd_b1m"):
            forward(1, 1, only=1, ends=False)
    first, last = (0, 1), (2, 3)
    for tiles_first, tiles_last in ((first, last), (last, first)):
        left_out(width - 2, tiles_first)
        left_out(1, tiles_last)
    for k in range(pair_dev):
        q = leading(c, k)
        with scope("pieces_a"):
            right_pieces(0, q)
        with scope("right"):
            right_moving(staying[0], q)
        if k == 0:
            with scope("left_c"):
                left(0)

                @pl.when(jnp.logical_not(has_prev))
                def _():
                    for at in range(pair_dev):
                        left_rows(2, at)
        with scope("right"):
            right_moving(staying[1], q)

    first, last = jnp.logical_not(has_prev), jnp.logical_not(has_next)

    def arrived(at, q):
        with scope("rows_arr"):
            @pl.when(has_prev | (at == width - 1))
            def _():
                left_rows(at, q)
        with scope("right"):
            right_moving(at, q)

    top, low = 0, width - 1
    arrived(jnp.where(last, low, top), jnp.where(last, 1, 0))
    arrived(jnp.where(first, top, low), jnp.where(last, 0, 1))
    for step in range(1, rows_n):
        with scope("fin_b"):
            finish(1, step)
    if square:
        with scope("via0"):
            right_relay(0)
            right_relay(1)
    arrived(jnp.where(first, low, top), jnp.where(last, 0, 1))
    arrived(jnp.where(last, top, low), jnp.where(last, 1, 0))
    with scope("pieces_b"):
        for p in range(pair_dev):
            right_pieces(1, p)
    with scope("right_local"):
        for at in staying + arriving:
            for j in (0, width - 1):
                right_kept(at, j)

    with scope("out_wait"):
        for slot in range(width):
            for layer in range(2):
                block_ref = out_ref.at[slot, :, pl.ds(layer * half, half), :]
                pltpu.make_async_copy(block_ref, block_ref, o_recv.at[slot, layer]).wait()
    drain(jr_send.at[0], jr_ref.at[:, :, pl.ds(0, (2 * cols_n - 1) * piece), :])
    drain(jo_send.at[0], jo_ref)
    drain(o_send.at[0], out_ref.at[pl.ds(0, width // 2)])
    for q, moved in ((0, left_end), (1, right_end)):
        drain(o_send.at[1 + q], out_ref.at[0, :, pl.ds(0, half), :], moved)
    for slot, moved in ((1, has_prev), (width - 2, has_next)):
        drain(lr_send.at[slot - 1], lr_ref.at[0], moved)
    with scope("send_wait"):
        for wait, condition in pending:
            if condition is None:
                wait()
            else:
                pl.when(condition)(wait)


def spread(size, x_ref, o_ref, buffer, in_sem, out_sem):
    width, block, tiles = size
    rows = buffer.shape[2]
    steps = block // rows

    def inward(k):
        i, at = k // steps, k % steps
        return pltpu.make_async_copy(x_ref.at[:, i, pl.ds(at * rows, rows), :], buffer.at[k], in_sem.at[k])

    def outward(k, j, tile):
        return pltpu.make_async_copy(
            buffer.at[k, j, :, pl.ds(tile * LANES, LANES)],
            o_ref.at[pl.ds(k * rows, rows), tile * width + j, 0, :], out_sem.at[k, j, tile],
        )

    every = range(width * steps)
    for k in every:
        inward(k).start()
    for k in every:
        inward(k).wait()
        for j in range(width):
            for tile in range(tiles):
                outward(k, j, tile).start()
    for k in every:
        for j in range(width):
            for tile in range(tiles):
                outward(k, j, tile).wait()


def shards(matrix, transforms):
    width, block, _, half = matrix.shape
    pair_dev = width // 2
    order = 2 * block
    rows_n, cols_n = lax.axis_size("row"), lax.axis_size("col")
    tiles = half // LANES
    raw_shape = (width * block, width * tiles, 1, LANES)
    own = transforms[0]
    piece = own.shape[1]
    f32, bf16 = jnp.float32, jnp.bfloat16

    raw = matrix.reshape(width * block, width, tiles, LANES).transpose(0, 2, 1, 3).reshape(raw_shape)
    any_space = pl.BlockSpec(memory_space=pl.ANY)
    dma = pltpu.SemaphoreType.DMA
    vmem = pltpu.VMEM
    by_piece = (2, pair_dev)
    by_unit = by_piece + (2 * piece, half)
    flops = 3 * 2 * 2 * width * half * order * width * block
    outs = pl.pallas_call(
        functools.partial(sweep, (rows_n, cols_n, pair_dev, width, block, half, piece)),
        name="sweep",
        out_shape=[
            jax.ShapeDtypeStruct((width, width, block, half), f32),
            jax.ShapeDtypeStruct(raw_shape, f32),
            jax.ShapeDtypeStruct((pair_dev, 2, order, half), f32),
            jax.ShapeDtypeStruct((cols_n,) + by_unit, f32),
            jax.ShapeDtypeStruct((rows_n, cols_n) + by_unit, f32),
            jax.ShapeDtypeStruct((width, width, half, block), f32),
            jax.ShapeDtypeStruct((2, 2, half, half), f32),
        ],
        in_specs=[any_space, any_space],
        out_specs=[any_space] * 7,
        scratch_shapes=[
            vmem((pair_dev, order, width * block), bf16),
            vmem((pair_dev, order, width * block), bf16),
            vmem((width, half, order), bf16),
            vmem((width, half, order), bf16),
            vmem((width, order, block), bf16),
            vmem((width, order, block), bf16),
            vmem((width, half, width * block), bf16),
            vmem((width, half, width * block), bf16),
            vmem((2 * width, half, block), f32),
            vmem((width * width, half, block), f32),
            vmem((pair_dev, piece, order), f32),
            vmem((2, ROWS, width * half), f32),
            vmem((4, pair_dev, 2 * piece, half), f32),
            vmem((2, half, block), f32),
            dma((2,)), dma((4 * pair_dev,)), dma((2,) + by_piece),
            dma((pair_dev,)), dma((pair_dev,)),
            dma((1,)), dma((cols_n, 2) + by_piece),
            dma((2, 2)),
            dma((rows_n, 2, 2)), dma((rows_n, 2) + by_piece),
            dma((rows_n, 2, 2)), dma((rows_n, 2) + by_piece),
            dma((rows_n, 2, 2)), dma((rows_n, 2, 2)), dma((cols_n,) + by_piece),
            dma((1,)), dma((cols_n,) + by_piece),
            dma((2,)), dma((width, width)),
            dma((3,)), dma((width, 2)),
            dma((2, 2)), dma((2, 2)),
        ],
        compiler_params=pltpu.CompilerParams(
            collective_id=0, has_side_effects=True, vmem_limit_bytes=VMEM_LIMIT
        ),
        cost_estimate=pl.CostEstimate(flops=flops, bytes_accessed=0, transcendentals=0),
    )(raw, own)
    blocks = outs[0]

    steps = width * block // ROWS
    result = pl.pallas_call(
        functools.partial(spread, (width, block, tiles)),
        name="spread",
        in_specs=[any_space],
        out_specs=any_space,
        out_shape=jax.ShapeDtypeStruct(raw_shape, f32),
        scratch_shapes=[
            vmem((steps, width, ROWS, half), f32), dma((steps,)), dma((steps, width, tiles)),
        ],
    )(blocks)
    result = result.reshape(width, block, tiles, width, LANES).transpose(0, 1, 3, 2, 4)
    return result.reshape(width, block, width, half)


def solution(mesh):
    return jax.shard_map(
        shards,
        mesh=mesh,
        in_specs=(P("row", None, "col", "layer"), P(None, "row", ("col", "layer"), None)),
        out_specs=P("row", None, "col", "layer"),
        check_vma=False,
    )
```
